256 devices in a mesh: row: 16 (over x, y), col: 16 (over z, core).
Axes of the slice: x: 4, y: 4, z: 8, core: 2. Of those that a mesh axis runs over, the one named last changes fastest.
Arguments:
- wrapped: float32 [1, 16384, 16384], P(None, 'row', 'col'), may hold values from -2.8 to 2.8
- col_steps: int32 [1, 16, 16], P(None, 'row', 'col'), may hold values from -2 to 2, as said below
- row_steps: int32 [1, 16, 16], P(None, 'row', 'col'), may hold values from -2 to 2, as said below
Outputs:
- unwrapped: float32 [1, 16384, 16384], P(None, 'row', 'col')
The draws below stay inside these ranges and needn't reach their ends.
Inputs may be any that keep to these rules, and one draw needn't show every extreme that they name: `col_steps`: nonzero whole numbers; the last tile column has no edge. `row_steps`: nonzero whole numbers; the last tile row has no edge.
All inputs are finite; a program needn't handle non-finite values.
Results may differ from the reference program's by a relative error of at most 0.0003.
Values sent between devices are 32-bit elements; how exact they have to be, the bound alone decides.
A program may use at most 64 MiB of HBM per device.

```python
import math
import jax
import jax.numpy as jnp
from jax import lax

FRAMES = 1
TILE_ROWS = 1024
TILE_COLS = 1024
ITERS = 2
IMAGE_ROWS = 16384
IMAGE_COLS = 16384
N_ROW = 16
N_COL = 16


TWO_PI = 2.0 * math.pi


def draw_wrapped(key, part):
    extent = (FRAMES, IMAGE_ROWS, IMAGE_COLS)
    levels = jax.random.randint(jax.random.fold_in(key, 1), extent, -3, 4)
    speckle = jax.random.randint(jax.random.fold_in(key, 2), extent, 0, 5)
    levels = jnp.where(speckle == 0, levels, 0)
    jitter = jnp.clip(0.04 * jax.random.normal(jax.random.fold_in(key, 3), extent, jnp.float32), -0.1, 0.1)
    return (TWO_PI / 7.0 * levels.astype(jnp.float32) + jitter).astype(jnp.float32)


def signed_steps(key):
    extent = (FRAMES, N_ROW, N_COL)
    magnitude = jax.random.randint(jax.random.fold_in(key, 1), extent, 1, 3)
    polarity = 2 * jax.random.randint(jax.random.fold_in(key, 2), extent, 0, 2) - 1
    return (magnitude * polarity).astype(jnp.int32)


def draw_col_steps(key, part):
    return signed_steps(jax.random.fold_in(key, 11))


def draw_row_steps(key, part):
    return signed_steps(jax.random.fold_in(key, 12))


def setup_inputs(seed: int = 0) -> dict:
    arg_keys = jax.random.split(jax.random.key(seed), 4)
    return {
        "wrapped": draw_wrapped(jax.random.fold_in(arg_keys[3], 71), 0),
        "col_steps": draw_col_steps(jax.random.fold_in(arg_keys[3], 71), 0),
        "row_steps": draw_row_steps(jax.random.fold_in(arg_keys[3], 71), 0),
    }


TWO_PI = 2.0 * math.pi


def wrap_diff(change):
    return change - TWO_PI * jnp.floor(change / TWO_PI + 0.5)


def unwrap_frame(inputs):
    wrapped, col_steps, row_steps = inputs
    grid_x = wrap_diff(wrapped[:, 1:] - wrapped[:, :-1])
    grid_x = jnp.concatenate([grid_x, jnp.zeros((IMAGE_ROWS, 1), grid_x.dtype)], axis=1)
    grid_y = wrap_diff(wrapped[1:, :] - wrapped[:-1, :])
    grid_y = jnp.concatenate([grid_y, jnp.zeros((1, IMAGE_COLS), grid_y.dtype)], axis=0)
    charge = (grid_x[:-1, :-1] + grid_y[:-1, 1:] - grid_x[1:, :-1] - grid_y[:-1, :-1]) / TWO_PI
    charge = jnp.pad(charge, ((1, 0), (1, 0)))
    weight = 1.0 / (1.0 + jnp.abs(charge))
    tiled_shape = (N_ROW, TILE_ROWS, N_COL, TILE_COLS)
    step_x = grid_x.reshape(tiled_shape)
    step_y = grid_y.reshape(tiled_shape)
    weight_tiles = weight.reshape(tiled_shape)
    along_cols = jnp.cumsum(step_x, axis=3) - step_x
    first_column = step_y[:, :, :, 0]
    downward = jnp.cumsum(first_column, axis=1) - first_column
    anchor = wrapped.reshape(tiled_shape)[:, 0, :, 0]
    current = (anchor[:, None, :] + downward)[:, :, :, None] + along_cols
    col_weight = weight_tiles[:, :, :, -1]
    cross_x = step_x[:, :, :, -1]
    row_weight = weight_tiles[:, -1, :, :]
    cross_y = step_y[:, -1, :, :]
    cycles_across = TWO_PI * col_steps.astype(jnp.float32)
    cycles_down = TWO_PI * row_steps.astype(jnp.float32)
    for sweep in range(ITERS):
        beyond_x = jnp.concatenate([current[:, :, 1:, 0], jnp.zeros((N_ROW, TILE_ROWS, 1), current.dtype)], axis=2)
        horizontal = jnp.sum(col_weight * (current[:, :, :, -1] + cross_x - beyond_x), axis=1) / jnp.sum(col_weight, axis=1)
        beyond_y = jnp.concatenate([current[1:, 0, :, :], jnp.zeros((1, N_COL, TILE_COLS), current.dtype)], axis=0)
        vertical = jnp.sum(row_weight * (current[:, -1, :, :] + cross_y - beyond_y), axis=2) / jnp.sum(row_weight, axis=2)
        horizontal = horizontal + cycles_across
        vertical = vertical + cycles_down
        prefix_across = jnp.cumsum(horizontal, axis=1) - horizontal
        prefix_down = jnp.cumsum(vertical, axis=0) - vertical
        offset = 0.5 * (prefix_across + prefix_across[0:1, :] + prefix_down + prefix_down[:, 0:1])
        current = current + offset[:, None, :, None]
    return (current / TWO_PI).reshape(IMAGE_ROWS, IMAGE_COLS)


def reference(wrapped, col_steps, row_steps):
    return lax.map(unwrap_frame, (wrapped, col_steps, row_steps))
```

```python
import functools
import math

import jax
import jax.numpy as jnp
from jax import lax
from jax.experimental import pallas as pl
from jax.experimental.pallas import tpu as pltpu
from jax.sharding import PartitionSpec as P

ITERS = 2
PER_CYCLE = 1.0 / (2.0 * math.pi)
MESH = pl.DeviceIdType.MESH
LANES = 128
STRIP = 32


def turns(change):
    return jnp.floor(change * PER_CYCLE + 0.5)


def positions(shape):
    return lax.broadcasted_iota(jnp.int32, shape, 0), lax.broadcasted_iota(jnp.int32, shape, 1)


def before(line, first):
    sub, lane = positions(line.shape)
    along = pltpu.roll(line, 1, 1)
    moved = jnp.where(lane == 0, pltpu.roll(along, 1, 0), along)
    return jnp.where((lane == 0) & (sub == 0), first, moved)


def line_turns(line):
    return turns(line - before(line, line))


def edge_weight(inner, outer, inner_first, outer_first, no_first):
    sub, lane = positions(inner.shape)
    cross = turns(outer - inner)
    cross_before = before(cross, turns(outer_first - inner_first))
    along_inner = turns(inner - before(inner, inner_first))
    along_outer = turns(outer - before(outer, outer_first))
    charge = jnp.abs(cross_before - cross + along_outer - along_inner)
    charge = jnp.where((lane == 0) & (sub == 0) & no_first, 0.0, charge)
    return 1.0 / (1.0 + charge)


def total(x):
    return jnp.sum(jnp.sum(x, axis=1, keepdims=True), axis=0, keepdims=True)


def kernel(
    n_row, n_col, wrapped, col_steps, row_steps, pre, offset,
    x, m, acc, mcol, tri, top, corner, own_col, own_last, beyond_col, below, corner_up, corner_left,
    jump_x, jump_y, seen_x, seen_y, sum_x, sum_y, first_x, first_y,
    in_sem, edge_sem, halo_send, halo_recv, x_send, x_recv, y_send, y_recv,
    first_x_send, first_x_recv, first_y_send, first_y_recv,
):
    r, c = lax.axis_index("row"), lax.axis_index("col")
    rows, cols = x.shape
    blocks = cols // LANES
    src = wrapped.at[0]

    get_top = pltpu.make_async_copy(src.at[pl.ds(0, 8), :], top, edge_sem.at[0])
    get_corner = pltpu.make_async_copy(
        src.at[pl.ds(rows - 8, 8), pl.ds(cols - LANES, LANES)], corner, edge_sem.at[1]
    )
    get_blocks = [
        pltpu.make_async_copy(
            src.at[:, pl.ds(LANES * j, LANES)], x.at[:, pl.ds(LANES * j, LANES)], in_sem.at[j]
        )
        for j in range(blocks)
    ]
    get_blocks[0].start()
    get_top.start()
    get_corner.start()
    for j in [blocks - 1] + list(range(1, blocks - 1)):
        get_blocks[j].start()

    barrier = pltpu.get_barrier_semaphore()
    for d in range(1, n_row):
        pl.semaphore_signal(
            barrier, inc=1, device_id={"row": lax.rem(r + d, n_row)}, device_id_type=MESH
        )
    for d in range(1, n_col):
        pl.semaphore_signal(
            barrier, inc=1, device_id={"col": lax.rem(c + d, n_col)}, device_id_type=MESH
        )

    get_blocks[0].wait()
    for s in range(8):
        turned = x[pl.ds(LANES * s, LANES), pl.ds(0, LANES)].T
        own_col[pl.ds(s, 1), :] = turned[0:1, :]
    get_top.wait()
    get_corner.wait()
    pl.semaphore_wait(barrier, n_row + n_col - 2)

    def halo(src_ref, dst_ref, k, device):
        return pltpu.make_async_remote_copy(
            src_ref=src_ref, dst_ref=dst_ref, send_sem=halo_send.at[k], recv_sem=halo_recv.at[k],
            device_id=device, device_id_type=MESH,
        )

    halos = [
        halo(own_col, beyond_col, 0, {"col": lax.rem(c + n_col - 1, n_col)}),
        halo(top.at[pl.ds(0, 1), :], below.at[pl.ds(0, 1), :], 1, {"row": lax.rem(r + n_row - 1, n_row)}),
        halo(corner, corner_up, 2, {"row": lax.rem(r + 1, n_row)}),
        halo(corner, corner_left, 3, {"col": lax.rem(c + 1, n_col)}),
    ]
    for copy in halos:
        copy.start()

    get_blocks[blocks - 1].wait()
    for s in range(8):
        turned = x[pl.ds(LANES * s, LANES), pl.ds(cols - LANES, LANES)].T
        own_last[pl.ds(s, 1), :] = turned[LANES - 2 : LANES - 1, :]
        own_last[pl.ds(8 + s, 1), :] = turned[LANES - 1 : LANES, :]
    for j in range(1, blocks - 1):
        get_blocks[j].wait()

    def strip(k, carry):
        at = pl.ds(pl.multiple_of(k * STRIP, STRIP), STRIP)
        here = x[at, :]
        n = turns(here - pltpu.roll(here, 1, 1))
        lane = lax.broadcasted_iota(jnp.int32, (STRIP, LANES), 1)
        parts = [n[:, LANES * j : LANES * (j + 1)] for j in range(blocks)]
        parts[0] = jnp.where(lane == 0, 0.0, parts[0])
        for j in range(blocks):
            m[at, pl.ds(LANES * j, LANES)] = parts[j].astype(jnp.bfloat16)
        while len(parts) > 1:
            parts = [a + b for a, b in zip(parts[::2], parts[1::2])]
        acc[at, :] = parts[0].astype(jnp.bfloat16)
        return carry

    lax.fori_loop(0, rows // STRIP, strip, 0, unroll=2)

    sub, lane = positions((8, LANES))
    flat_totals = lax.dot_general(
        jnp.ones((8, LANES), jnp.bfloat16), acc[...], (((1,), (1,)), ((), ())),
        preferred_element_type=jnp.float32,
    )
    row_totals = jnp.zeros((8, LANES), jnp.float32)
    for s in range(8):
        row_totals = jnp.where(sub == s, flat_totals[:, LANES * s : LANES * (s + 1)], row_totals)

    def row_line(ref, i):
        return jnp.concatenate([ref[i : i + 1, LANES * s : LANES * (s + 1)] for s in range(8)], axis=0)

    col0 = own_col[...]
    col_in, col_out = own_last[0:8, :], own_last[8:16, :]
    row_in, row_out = row_line(x, rows - 2), row_line(x, rows - 1)

    for copy in halos:
        copy.wait_recv()
    right_col = beyond_col[...]
    below_row = row_line(below, 0)

    weight_x = edge_weight(
        col_in, col_out, corner_up[7:8, LANES - 2 : LANES - 1], corner_up[7:8, LANES - 1 : LANES], r == 0
    )
    weight_y = edge_weight(
        row_in, row_out, corner_left[6:7, LANES - 1 : LANES], corner_left[7:8, LANES - 1 : LANES], c == 0
    )
    stack = jnp.concatenate([line_turns(v) for v in (right_col, col0, below_row, row_out)], axis=0)
    sub32, _ = positions(stack.shape)
    sub32 = lax.rem(sub32, 8)
    carry = jnp.where(sub32 >= 1, pltpu.roll(stack, 1, 0), 0.0)
    for step in (1, 2, 4):
        carry = carry + jnp.where(sub32 >= step, pltpu.roll(carry, step, 0), 0.0)
    ka, kb = positions((2 * LANES, LANES))
    prefix = jnp.dot(
        jnp.concatenate([stack, carry], axis=1).astype(jnp.bfloat16),
        ((ka <= kb) | (ka >= LANES)).astype(jnp.float32).astype(jnp.bfloat16),
        preferred_element_type=jnp.float32,
    )
    down = prefix[8:16]
    miss_x = prefix[0:8] - down - row_totals - turns(right_col - col_out)
    miss_y = prefix[16:24] - prefix[24:32] - down[7:8, LANES - 1 : LANES] - turns(below_row - row_out)
    mean_x = total(weight_x * miss_x) / total(weight_x) + col_steps[0, 0, 0].astype(jnp.float32)
    mean_y = total(weight_y * miss_y) / total(weight_y) + row_steps[0, 0, 0].astype(jnp.float32)
    jump_x[...] = jnp.broadcast_to(mean_x, (8, LANES))
    jump_y[...] = jnp.broadcast_to(mean_y, (8, LANES))

    def to_row(d):
        return pltpu.make_async_remote_copy(
            src_ref=jump_y.at[pl.ds(0, 1), :], dst_ref=seen_y.at[pl.ds(r, 1), :],
            send_sem=y_send.at[d - 1], recv_sem=y_recv.at[d - 1],
            device_id={"row": lax.rem(r + d, n_row)}, device_id_type=MESH,
        )

    def to_col(d):
        return pltpu.make_async_remote_copy(
            src_ref=jump_x.at[pl.ds(0, 1), :], dst_ref=seen_x.at[pl.ds(c, 1), :],
            send_sem=x_send.at[d - 1], recv_sem=x_recv.at[d - 1],
            device_id={"col": lax.rem(c + d, n_col)}, device_id_type=MESH,
        )

    first = [to_row(d) for d in range(1, n_row)] + [to_col(d) for d in range(1, n_col)]
    for copy in first:
        copy.start()

    for s in range(8):
        mcol[pl.ds(LANES * s, LANES), :] = jnp.broadcast_to(down[s : s + 1, :], (LANES, LANES)).T
    ta, tb = positions(tri.shape)
    tri[...] = (ta - (rows - 256) <= tb).astype(jnp.float32).astype(jnp.bfloat16)

    def finish(k, carry):
        at = pl.ds(pl.multiple_of(k * 256, 256), 256)
        base = mcol[at, :]
        base = jnp.concatenate([base, base], axis=1)
        for j in range(cols // 256):
            width = 256 * (j + 1)
            counted = jnp.dot(
                m[at, pl.ds(0, width)], tri[pl.ds(rows - width, width), :],
                preferred_element_type=jnp.float32,
            )
            here = pl.ds(256 * j, 256)
            pre[at, here] = x[at, here] * PER_CYCLE - counted - base
        return carry

    lax.fori_loop(0, rows // 256, finish, 0)

    for copy in first:
        copy.wait_recv()
    seen = lax.broadcasted_iota(jnp.int32, (n_col, LANES), 0)
    across = jnp.sum(jnp.where(seen < c, seen_x[...], 0.0), axis=0, keepdims=True)
    seen = lax.broadcasted_iota(jnp.int32, (n_row, LANES), 0)
    downs = jnp.sum(jnp.where(seen < r, seen_y[...], 0.0), axis=0, keepdims=True)
    sum_x[...] = jnp.broadcast_to(across, (8, LANES))
    sum_y[...] = jnp.broadcast_to(downs, (8, LANES))

    def first_row(t):
        return pltpu.make_async_remote_copy(
            src_ref=sum_x.at[pl.ds(0, 1), :], dst_ref=first_x.at[pl.ds(0, 1), :],
            send_sem=first_x_send.at[t - 1], recv_sem=first_x_recv.at[0],
            device_id={"row": t}, device_id_type=MESH,
        )

    def first_col(t):
        return pltpu.make_async_remote_copy(
            src_ref=sum_y.at[pl.ds(0, 1), :], dst_ref=first_y.at[pl.ds(0, 1), :],
            send_sem=first_y_send.at[t - 1], recv_sem=first_y_recv.at[0],
            device_id={"col": t}, device_id_type=MESH,
        )

    @pl.when(r == 0)
    def _():
        for t in range(1, n_row):
            first_row(t).start()

    @pl.when(c == 0)
    def _():
        for t in range(1, n_col):
            first_col(t).start()

    @pl.when(r != 0)
    def _():
        first_row(1).wait_recv()

    @pl.when(c != 0)
    def _():
        first_col(1).wait_recv()

    across_top = jnp.where(r == 0, across, first_x[0:1, :])
    downs_left = jnp.where(c == 0, downs, first_y[0:1, :])

    mine = top_tile = left_tile = origin = jnp.zeros((1, LANES), jnp.float32)
    for sweep in range(ITERS):
        prefix_across = across + left_tile - mine
        prefix_across_top = across_top + origin - top_tile
        prefix_down = downs + top_tile - mine
        prefix_down_left = downs_left + origin - left_tile
        mine = mine + 0.5 * (prefix_across + prefix_across_top + prefix_down + prefix_down_left)
        top_tile = top_tile + 0.5 * (prefix_across_top + prefix_across_top)
        left_tile = left_tile + 0.5 * (prefix_down_left + prefix_down_left)
    offset[...] = jnp.broadcast_to(mine, (8, LANES))

    for copy in halos + first:
        copy.wait_send()

    @pl.when(r == 0)
    def _():
        for t in range(1, n_row):
            first_row(t).wait_send()

    @pl.when(c == 0)
    def _():
        for t in range(1, n_col):
            first_col(t).wait_send()


def on_device(n_row, n_col, wrapped, col_steps, row_steps):
    _, rows, cols = wrapped.shape
    f32 = jnp.float32
    line = pltpu.VMEM((8, LANES), f32)
    dma = pltpu.SemaphoreType.DMA
    in_hbm = pl.BlockSpec(memory_space=pltpu.HBM)
    in_smem = pl.BlockSpec(memory_space=pltpu.SMEM)
    in_vmem = pl.BlockSpec(memory_space=pltpu.VMEM)
    pre, offset = pl.pallas_call(
        functools.partial(kernel, n_row, n_col),
        out_shape=(jax.ShapeDtypeStruct((rows, cols), f32), jax.ShapeDtypeStruct((8, LANES), f32)),
        in_specs=[in_hbm, in_smem, in_smem],
        out_specs=(in_vmem, in_vmem),
        scratch_shapes=[
            pltpu.VMEM((rows, cols), f32),
            pltpu.VMEM((rows, cols), jnp.bfloat16),
            pltpu.VMEM((rows, LANES), jnp.bfloat16),
            pltpu.VMEM((rows, LANES), f32),
            pltpu.VMEM((rows, 256), jnp.bfloat16),
            pltpu.VMEM((8, cols), f32),
            line,
            line,
            pltpu.VMEM((16, LANES), f32),
            line,
            pltpu.VMEM((8, cols), f32),
            line,
            line,
            line,
            line,
            pltpu.VMEM((n_col, LANES), f32),
            pltpu.VMEM((n_row, LANES), f32),
            line,
            line,
            line,
            line,
            dma((cols // LANES,)),
            dma((2,)),
            dma((4,)),
            dma((4,)),
            dma((n_col - 1,)),
            dma((n_col - 1,)),
            dma((n_row - 1,)),
            dma((n_row - 1,)),
            dma((n_row - 1,)),
            dma((1,)),
            dma((n_col - 1,)),
            dma((1,)),
        ],
        compiler_params=pltpu.CompilerParams(
            collective_id=0, has_side_effects=True, vmem_limit_bytes=24 * 1024 * 1024
        ),
    )(pltpu.with_memory_space_constraint(wrapped, pltpu.HBM), col_steps, row_steps)
    return (pre + offset[0:1, 0:1])[None]


def solution(mesh):
    spec = P(None, "row", "col")
    return jax.shard_map(
        functools.partial(on_device, mesh.shape["row"], mesh.shape["col"]),
        mesh=mesh, in_specs=(spec, spec, spec), out_specs=spec, check_vma=False,
    )
```

```python
import functools
import math

import jax
import jax.numpy as jnp
from jax import lax
from jax.experimental import pallas as pl
from jax.experimental.pallas import tpu as pltpu
from jax.sharding import PartitionSpec as P

ITERS = 2
PER_CYCLE = 1.0 / (2.0 * math.pi)
MESH = pl.DeviceIdType.MESH
LANES = 128
STRIP = 16
UNROLL = 16
PIECES = 8
NEAR = 3


def turns(change):
    return jnp.floor(change * PER_CYCLE + 0.5)


def positions(shape):
    return lax.broadcasted_iota(jnp.int32, shape, 0), lax.broadcasted_iota(jnp.int32, shape, 1)


def before(line, first):
    sub, lane = positions(line.shape)
    along = pltpu.roll(line, 1, 1)
    moved = jnp.where(lane == 0, pltpu.roll(along, 1, 0), along)
    return jnp.where((lane == 0) & (sub == 0), first, moved)


def line_turns(line):
    return turns(line - before(line, line))


def edge_weight(inner, outer, inner_first, outer_first, no_first):
    sub, lane = positions(inner.shape)
    cross = turns(outer - inner)
    cross_before = before(cross, turns(outer_first - inner_first))
    along_inner = turns(inner - before(inner, inner_first))
    along_outer = turns(outer - before(outer, outer_first))
    charge = jnp.abs(cross_before - cross + along_outer - along_inner)
    charge = jnp.where((lane == 0) & (sub == 0) & no_first, 0.0, charge)
    return 1.0 / (1.0 + charge)


def total(x):
    return jnp.sum(jnp.sum(x, axis=1, keepdims=True), axis=0, keepdims=True)


def kernel(
    n_row, n_col, wrapped, col_steps, row_steps, pre, offset,
    x, m, acc, mcol, tri, top, corner, own_col, own_last, beyond_col, below, corner_up, corner_left,
    jump_x, jump_y, seen_x, seen_y, sum_x, sum_y, first_x, first_y,
    in_sem, edge_sem, halo_send, halo_recv, ready_x, ready_y, x_send, x_recv, y_send, y_recv,
    first_x_send, first_x_recv, first_y_send, first_y_recv,
):
    r, c = lax.axis_index("row"), lax.axis_index("col")
    rows, cols = x.shape
    blocks = cols // LANES
    src = wrapped.at[0]

    get_top = pltpu.make_async_copy(src.at[pl.ds(0, 8), :], top, edge_sem.at[0])
    get_corner = pltpu.make_async_copy(
        src.at[pl.ds(rows - 8, 8), pl.ds(cols - LANES, LANES)], corner, edge_sem.at[1]
    )
    get_blocks = [
        pltpu.make_async_copy(
            src.at[:, pl.ds(LANES * j, LANES)], x.at[:, pl.ds(LANES * j, LANES)], in_sem.at[j]
        )
        for j in range(blocks)
    ]
    get_top.start()
    get_corner.start()
    get_blocks[0].start()
    for j in [blocks - 1] + list(range(1, blocks - 1)):
        get_blocks[j].start()

    barrier = pltpu.get_barrier_semaphore()

    def greet(device):
        pl.semaphore_signal(barrier, inc=1, device_id=device, device_id_type=MESH)

    @pl.when(c > 0)
    def _():
        greet({"col": c - 1})

    @pl.when(r > 0)
    def _():
        greet({"row": r - 1})

    @pl.loop(r + 1, n_row)
    def _(t):
        greet({"row": t})

    @pl.loop(c + 1, n_col)
    def _(t):
        greet({"col": t})

    get_blocks[0].wait()
    for s in range(8):
        turned = x[pl.ds(LANES * s, LANES), pl.ds(0, LANES)].T
        own_col[pl.ds(s, 1), :] = turned[0:1, :]
    get_top.wait()
    get_corner.wait()
    has_right, has_below = c < n_col - 1, r < n_row - 1
    pl.semaphore_wait(barrier, r + c + has_right.astype(jnp.int32) + has_below.astype(jnp.int32))

    def halo(src_ref, dst_ref, k, device):
        return pltpu.make_async_remote_copy(
            src_ref=src_ref, dst_ref=dst_ref, send_sem=halo_send.at[k], recv_sem=halo_recv.at[k],
            device_id=device, device_id_type=MESH,
        )

    to_left = halo(own_col, beyond_col, 0, {"col": lax.rem(c + n_col - 1, n_col)})
    to_above = halo(top.at[pl.ds(0, 1), :], below.at[pl.ds(0, 1), :], 1, {"row": lax.rem(r + n_row - 1, n_row)})
    to_below = halo(corner, corner_up, 2, {"row": lax.rem(r + 1, n_row)})
    to_right = halo(corner, corner_left, 3, {"col": lax.rem(c + 1, n_col)})
    sends = ((c > 0, to_left), (r > 0, to_above), (has_below, to_below), (has_right, to_right))
    arrivals = ((has_right, to_left), (has_below, to_above), (r > 0, to_below), (c > 0, to_right))

    for holds, copy in sends:
        @pl.when(holds)
        def _(copy=copy):
            copy.start()

    @pl.loop(0, r)
    def _(k):
        pl.semaphore_signal(
            ready_y.at[r], inc=1, device_id={"row": r - 1 - k}, device_id_type=MESH
        )

    @pl.loop(0, c)
    def _(k):
        pl.semaphore_signal(
            ready_x.at[c], inc=1, device_id={"col": c - 1 - k}, device_id_type=MESH
        )

    get_blocks[blocks - 1].wait()
    for s in range(8):
        turned = x[pl.ds(LANES * s, LANES), pl.ds(cols - LANES, LANES)].T
        own_last[pl.ds(s, 1), :] = turned[LANES - 2 : LANES - 1, :]
        own_last[pl.ds(8 + s, 1), :] = turned[LANES - 1 : LANES, :]
    for j in range(1, blocks - 1):
        get_blocks[j].wait()

    @pl.loop(0, rows // STRIP, unroll=UNROLL)
    def _(k):
        at = pl.ds(pl.multiple_of(k * STRIP, STRIP), STRIP)
        lane = lax.broadcasted_iota(jnp.int32, (STRIP, LANES), 1)
        counts, moved = [], None
        for j in range(blocks):
            here = x[at, pl.ds(LANES * j, LANES)]
            last, moved = moved, pltpu.roll(here, 1, 1)
            back = moved if j == 0 else jnp.where(lane == 0, last, moved)
            n = turns(here - back)
            n = jnp.where(lane == 0, 0.0, n) if j == 0 else n
            m[j, at, :] = n.astype(jnp.bfloat16)
            counts.append(n)
        while len(counts) > 1:
            counts = [a + b for a, b in zip(counts[::2], counts[1::2])]
        acc[at, :] = counts[0].astype(jnp.bfloat16)

    sub, lane = positions((8, LANES))
    flat_totals = lax.dot_general(
        jnp.ones((8, LANES), jnp.bfloat16), acc[...], (((1,), (1,)), ((), ())),
        preferred_element_type=jnp.float32,
    )
    row_totals = jnp.zeros((8, LANES), jnp.float32)
    for s in range(8):
        row_totals = jnp.where(sub == s, flat_totals[:, LANES * s : LANES * (s + 1)], row_totals)

    def row_line(ref, i):
        return jnp.concatenate([ref[i : i + 1, LANES * s : LANES * (s + 1)] for s in range(8)], axis=0)

    col0 = own_col[...]
    col_in, col_out = own_last[0:8, :], own_last[8:16, :]
    row_in, row_out = row_line(x, rows - 2), row_line(x, rows - 1)

    for holds, copy in arrivals:
        @pl.when(holds)
        def _(copy=copy):
            copy.wait_recv()

    right_col = beyond_col[...]
    below_row = row_line(below, 0)
    weight_x = edge_weight(
        col_in, col_out, corner_up[7:8, LANES - 2 : LANES - 1], corner_up[7:8, LANES - 1 : LANES], r == 0
    )
    weight_y = edge_weight(
        row_in, row_out, corner_left[6:7, LANES - 1 : LANES], corner_left[7:8, LANES - 1 : LANES], c == 0
    )
    stack = jnp.concatenate([line_turns(v) for v in (right_col, col0, below_row, row_out)], axis=0)
    sub32, _ = positions(stack.shape)
    sub32 = lax.rem(sub32, 8)
    carry = jnp.where(sub32 >= 1, pltpu.roll(stack, 1, 0), 0.0)
    for step in (1, 2, 4):
        carry = carry + jnp.where(sub32 >= step, pltpu.roll(carry, step, 0), 0.0)
    ka, kb = positions((2 * LANES, LANES))
    prefix = jnp.dot(
        jnp.concatenate([stack, carry], axis=1).astype(jnp.bfloat16),
        ((ka <= kb) | (ka >= LANES)).astype(jnp.float32).astype(jnp.bfloat16),
        preferred_element_type=jnp.float32,
    )
    down = prefix[8:16]
    miss_x = prefix[0:8] - down - row_totals - turns(right_col - col_out)
    miss_y = prefix[16:24] - prefix[24:32] - down[7:8, LANES - 1 : LANES] - turns(below_row - row_out)
    mean_x = total(weight_x * miss_x) / total(weight_x) + col_steps[0, 0, 0].astype(jnp.float32)
    mean_y = total(weight_y * miss_y) / total(weight_y) + row_steps[0, 0, 0].astype(jnp.float32)
    jump_x[...] = jnp.broadcast_to(mean_x, (8, LANES))
    jump_y[...] = jnp.broadcast_to(mean_y, (8, LANES))

    def to_row(t):
        return pltpu.make_async_remote_copy(
            src_ref=jump_y.at[pl.ds(0, 1), :], dst_ref=seen_y.at[pl.ds(r, 1), :],
            send_sem=y_send.at[t], recv_sem=y_recv.at[r],
            device_id={"row": t}, device_id_type=MESH,
        )

    def to_col(t):
        return pltpu.make_async_remote_copy(
            src_ref=jump_x.at[pl.ds(0, 1), :], dst_ref=seen_x.at[pl.ds(c, 1), :],
            send_sem=x_send.at[t], recv_sem=x_recv.at[c],
            device_id={"col": t}, device_id_type=MESH,
        )

    def send_y(t):
        pl.semaphore_wait(ready_y.at[t], 1)
        to_row(t).start()

    def send_x(t):
        pl.semaphore_wait(ready_x.at[t], 1)
        to_col(t).start()

    stop_x = jnp.where(c < n_col // 4, n_col // 2, n_col)
    near_y, near_x = jnp.minimum(r + 1 + NEAR, n_row), jnp.minimum(c + 1 + NEAR, stop_x)
    pl.loop(r + 1, near_y)(send_y)
    pl.loop(c + 1, near_x)(send_x)

    for s in range(8):
        mcol[pl.ds(LANES * s, LANES), :] = jnp.broadcast_to(down[s : s + 1, :], (LANES, LANES)).T
    ta, tb = positions(tri.shape)
    tri[...] = ((ta <= tb) | (tb >= 2 * LANES)).astype(jnp.float32).astype(jnp.bfloat16)

    @pl.loop(0, rows // 256)
    def _(k):
        at = pl.ds(pl.multiple_of(k * 256, 256), 256)
        base = mcol[at, :]
        for j in range(blocks // 2):
            counted = jnp.dot(
                jnp.concatenate([m[2 * j, at, :], m[2 * j + 1, at, :]], axis=1), tri[...],
                preferred_element_type=jnp.float32,
            )
            for h in range(2):
                here = pl.ds(LANES * (2 * j + h), LANES)
                pre[at, here] = x[at, here] * PER_CYCLE - counted[:, LANES * h : LANES * (h + 1)] - base
            base = base + counted[:, 2 * LANES :]

    pl.loop(near_y, n_row)(send_y)
    pl.loop(near_x, stop_x)(send_x)

    @pl.loop(0, r)
    def _(k):
        pltpu.make_async_remote_copy(
            src_ref=jump_y.at[pl.ds(0, 1), :], dst_ref=seen_y.at[pl.ds(k, 1), :],
            send_sem=y_send.at[k], recv_sem=y_recv.at[k],
            device_id={"row": k}, device_id_type=MESH,
        ).wait_recv()

    @pl.loop(0, c)
    def _(k):
        pltpu.make_async_remote_copy(
            src_ref=jump_x.at[pl.ds(0, 1), :], dst_ref=seen_x.at[pl.ds(k, 1), :],
            send_sem=x_send.at[k], recv_sem=x_recv.at[k],
            device_id={"col": k}, device_id_type=MESH,
        ).wait_recv()

    seen = lax.broadcasted_iota(jnp.int32, (n_col, LANES), 0)
    across = jnp.sum(jnp.where(seen < c, seen_x[...], 0.0), axis=0, keepdims=True)
    seen = lax.broadcasted_iota(jnp.int32, (n_row, LANES), 0)
    downs = jnp.sum(jnp.where(seen < r, seen_y[...], 0.0), axis=0, keepdims=True)
    sum_x[...] = jnp.broadcast_to(across, (8, LANES))
    sum_y[...] = jnp.broadcast_to(downs, (8, LANES))

    def first_row(t):
        return pltpu.make_async_remote_copy(
            src_ref=sum_x.at[pl.ds(0, 1), :], dst_ref=first_x.at[pl.ds(0, 1), :],
            send_sem=first_x_send.at[t], recv_sem=first_x_recv.at[0],
            device_id={"row": t}, device_id_type=MESH,
        )

    def first_col(t):
        return pltpu.make_async_remote_copy(
            src_ref=sum_y.at[pl.ds(0, 1), :], dst_ref=first_y.at[pl.ds(0, 1), :],
            send_sem=first_y_send.at[t], recv_sem=first_y_recv.at[0],
            device_id={"col": t}, device_id_type=MESH,
        )

    @pl.when(r == 0)
    def _():
        @pl.loop(1, n_row)
        def _(t):
            first_row(t).start()

    head_y = jnp.where(c == 0, stop_x, 1)

    @pl.loop(1, head_y)
    def _(t):
        first_col(t).start()

    @pl.loop(stop_x, n_col)
    def _(t):
        send_x(t)

        @pl.when(c == 0)
        def _():
            first_col(t).start()

    @pl.when(r != 0)
    def _():
        first_row(1).wait_recv()

    @pl.when(c != 0)
    def _():
        first_col(1).wait_recv()

    across_top = jnp.where(r == 0, across, first_x[0:1, :])
    downs_left = jnp.where(c == 0, downs, first_y[0:1, :])

    mine = top_tile = left_tile = origin = jnp.zeros((1, LANES), jnp.float32)
    for sweep in range(ITERS):
        prefix_across = across + left_tile - mine
        prefix_across_top = across_top + origin - top_tile
        prefix_down = downs + top_tile - mine
        prefix_down_left = downs_left + origin - left_tile
        mine = mine + 0.5 * (prefix_across + prefix_across_top + prefix_down + prefix_down_left)
        top_tile = top_tile + 0.5 * (prefix_across_top + prefix_across_top)
        left_tile = left_tile + 0.5 * (prefix_down_left + prefix_down_left)
    offset[...] = jnp.broadcast_to(mine, (8, LANES))

    for holds, copy in sends:
        @pl.when(holds)
        def _(copy=copy):
            copy.wait_send()

    @pl.loop(r + 1, n_row)
    def _(t):
        to_row(t).wait_send()

    @pl.loop(c + 1, n_col)
    def _(t):
        to_col(t).wait_send()

    @pl.when(r == 0)
    def _():
        @pl.loop(1, n_row)
        def _(t):
            first_row(t).wait_send()

    @pl.when(c == 0)
    def _():
        @pl.loop(1, n_col)
        def _(t):
            first_col(t).wait_send()


def add_offset(pre, offset, out, done, sem):
    piece = pre.shape[0] // PIECES
    copies = []
    for k in range(PIECES):
        at = pl.ds(k * piece, piece)
        done[at, :] = pre[at, :] + offset[0:1, 0:1]
        copy = pltpu.make_async_copy(done.at[at, :], out.at[0, at, :], sem.at[k])
        copy.start()
        copies.append(copy)
    for copy in copies:
        copy.wait()


def on_device(n_row, n_col, wrapped, col_steps, row_steps):
    _, rows, cols = wrapped.shape
    f32 = jnp.float32
    line = pltpu.VMEM((8, LANES), f32)
    dma = pltpu.SemaphoreType.DMA
    in_hbm = pl.BlockSpec(memory_space=pltpu.HBM)
    in_smem = pl.BlockSpec(memory_space=pltpu.SMEM)
    in_vmem = pl.BlockSpec(memory_space=pltpu.VMEM)
    pre, offset = pl.pallas_call(
        functools.partial(kernel, n_row, n_col),
        out_shape=(jax.ShapeDtypeStruct((rows, cols), f32), jax.ShapeDtypeStruct((8, LANES), f32)),
        in_specs=[in_hbm, in_smem, in_smem],
        out_specs=(in_vmem, in_vmem),
        scratch_shapes=[
            pltpu.VMEM((rows, cols), f32),
            pltpu.VMEM((cols // LANES, rows, LANES), jnp.bfloat16),
            pltpu.VMEM((rows, LANES), jnp.bfloat16),
            pltpu.VMEM((rows, LANES), f32),
            pltpu.VMEM((2 * LANES, 3 * LANES), jnp.bfloat16),
            pltpu.VMEM((8, cols), f32),
            line,
            line,
            pltpu.VMEM((16, LANES), f32),
            line,
            pltpu.VMEM((8, cols), f32),
            line,
            line,
            line,
            line,
            pltpu.VMEM((n_col, LANES), f32),
            pltpu.VMEM((n_row, LANES), f32),
            line,
            line,
            line,
            line,
            dma((cols // LANES,)),
            dma((2,)),
            dma((4,)),
            dma((4,)),
            pltpu.SemaphoreType.REGULAR((n_col,)),
            pltpu.SemaphoreType.REGULAR((n_row,)),
            dma((n_col,)),
            dma((n_col,)),
            dma((n_row,)),
            dma((n_row,)),
            dma((n_row,)),
            dma((1,)),
            dma((n_col,)),
            dma((1,)),
        ],
        compiler_params=pltpu.CompilerParams(
            collective_id=0, has_side_effects=True, vmem_limit_bytes=24 * 1024 * 1024
        ),
    )(pltpu.with_memory_space_constraint(wrapped, pltpu.HBM), col_steps, row_steps)
    out = pl.pallas_call(
        add_offset,
        out_shape=jax.ShapeDtypeStruct((1, rows, cols), f32),
        in_specs=[in_vmem, in_vmem],
        out_specs=in_hbm,
        scratch_shapes=[pltpu.VMEM((rows, cols), f32), dma((PIECES,))],
        compiler_params=pltpu.CompilerParams(vmem_limit_bytes=8 * 1024 * 1024),
    )(pre, offset)
    return out


def solution(mesh):
    spec = P(None, "row", "col")
    return jax.shard_map(
        functools.partial(on_device, mesh.shape["row"], mesh.shape["col"]),
        mesh=mesh, in_specs=(spec, spec, spec), out_specs=spec, check_vma=False,
    )
```

```python
import functools
import math

import jax
import jax.numpy as jnp
from jax import lax
from jax.experimental import pallas as pl
from jax.experimental.pallas import tpu as pltpu
from jax.sharding import PartitionSpec as P

ITERS = 2
PER_CYCLE = 1.0 / (2.0 * math.pi)
MESH = pl.DeviceIdType.MESH
LANES = 128
STRIP = 16
PARTS = (256, 256, 256, 256)
MEET = 2
PIECES = 8
NEAR = 3


def turns(change):
    return jnp.floor(change * PER_CYCLE + 0.5)


def positions(shape):
    return lax.broadcasted_iota(jnp.int32, shape, 0), lax.broadcasted_iota(jnp.int32, shape, 1)


def before(line, first):
    sub, lane = positions(line.shape)
    along = pltpu.roll(line, 1, 1)
    moved = jnp.where(lane == 0, pltpu.roll(along, 1, 0), along)
    return jnp.where((lane == 0) & (sub == 0), first, moved)


def line_turns(line):
    return turns(line - before(line, line))


def edge_weight(inner, outer, inner_first, outer_first, no_first):
    sub, lane = positions(inner.shape)
    cross = turns(outer - inner)
    cross_before = before(cross, turns(outer_first - inner_first))
    along_inner = turns(inner - before(inner, inner_first))
    along_outer = turns(outer - before(outer, outer_first))
    charge = jnp.abs(cross_before - cross + along_outer - along_inner)
    charge = jnp.where((lane == 0) & (sub == 0) & no_first, 0.0, charge)
    return 1.0 / (1.0 + charge)


def total(x):
    return jnp.sum(jnp.sum(x, axis=1, keepdims=True), axis=0, keepdims=True)


def running_turns(lines):
    stack = jnp.concatenate([line_turns(v) for v in lines], axis=0)
    sub, _ = positions(stack.shape)
    sub = lax.rem(sub, 8)
    carry = jnp.where(sub >= 1, pltpu.roll(stack, 1, 0), 0.0)
    for step in (1, 2, 4):
        carry = carry + jnp.where(sub >= step, pltpu.roll(carry, step, 0), 0.0)
    ka, kb = positions((2 * LANES, LANES))
    prefix = jnp.dot(
        jnp.concatenate([stack, carry], axis=1).astype(jnp.bfloat16),
        ((ka <= kb) | (ka >= LANES)).astype(jnp.float32).astype(jnp.bfloat16),
        preferred_element_type=jnp.float32,
    )
    return [prefix[8 * k : 8 * k + 8] for k in range(len(lines))]


def row_line(ref, i):
    return jnp.concatenate([ref[i : i + 1, LANES * s : LANES * (s + 1)] for s in range(8)], axis=0)


def kernel(
    n_row, n_col, wrapped, col_steps, row_steps, pre, offset,
    x, m, acc, mcol, tri, own_col, bottom, edge_x, edge_y, left, above, corner,
    jump_x, jump_y, seen_x, seen_y, first_x, first_y,
    in_sem, edge_sem, halo_send, halo_recv, ready_x, ready_y, x_send, x_recv, y_send, y_recv, first_recv,
):
    r, c = lax.axis_index("row"), lax.axis_index("col")
    rows, cols = x.shape
    blocks = cols // LANES
    src = wrapped.at[0]

    get_bottom = pltpu.make_async_copy(src.at[pl.ds(rows - 8, 8), :], edge_y, edge_sem.at[0])
    get_corner = pltpu.make_async_copy(
        src.at[pl.ds(rows - 8, 8), pl.ds(cols - LANES, LANES)], bottom, edge_sem.at[1]
    )
    get_parts = [
        pltpu.make_async_copy(
            src.at[pl.ds(sum(PARTS[:k]), part), :], x.at[pl.ds(sum(PARTS[:k]), part), :], in_sem.at[k]
        )
        for k, part in enumerate(PARTS)
    ]
    for copy in get_parts[:1] + [get_bottom, get_corner] + get_parts[1:]:
        copy.start()

    barrier = pltpu.get_barrier_semaphore()

    def greet(device):
        pl.semaphore_signal(barrier, inc=1, device_id=device, device_id_type=MESH)

    @pl.when(c > 0)
    def _():
        greet({"col": c - 1})

    @pl.when(r > 0)
    def _():
        greet({"row": r - 1})

    @pl.when((r > 0) & (c > 0))
    def _():
        greet({"row": r - 1, "col": c - 1})

    @pl.loop(r + 1, n_row)
    def _(t):
        greet({"row": t})

    @pl.loop(c + 1, n_col)
    def _(t):
        greet({"col": t})

    has_right, has_below = c < n_col - 1, r < n_row - 1
    touching = has_right.astype(jnp.int32) + has_below.astype(jnp.int32)
    touching = touching + (has_right & has_below).astype(jnp.int32)

    def meet():
        pl.semaphore_wait(barrier, r + c + touching)

        @pl.loop(0, r)
        def _(k):
            pl.semaphore_signal(
                ready_y.at[r], inc=1, device_id={"row": r - 1 - k}, device_id_type=MESH
            )

        @pl.loop(0, c)
        def _(k):
            pl.semaphore_signal(
                ready_x.at[c], inc=1, device_id={"col": c - 1 - k}, device_id_type=MESH
            )

    first = 0
    for k, part in enumerate(PARTS):
        if k == MEET:
            meet()
        get_parts[k].wait()
        for s in range(first // LANES, (first + part) // LANES):
            at = pl.ds(LANES * s, LANES)
            own_col[pl.ds(s, 1), :] = x[at, pl.ds(0, LANES)].T[0:1, :]
            turned = x[at, pl.ds(cols - LANES, LANES)].T
            edge_x[pl.ds(s, 1), :] = turned[LANES - 2 : LANES - 1, :]
            edge_x[pl.ds(8 + s, 1), :] = turned[LANES - 1 : LANES, :]
        for q in range(first // STRIP, (first + part) // STRIP):
            at = pl.ds(STRIP * q, STRIP)
            lane = lax.broadcasted_iota(jnp.int32, (STRIP, LANES), 1)
            counts, moved = [], None
            for j in range(blocks):
                here = x[at, pl.ds(LANES * j, LANES)]
                last, moved = moved, pltpu.roll(here, 1, 1)
                back = moved if j == 0 else jnp.where(lane == 0, last, moved)
                n = turns(here - back)
                n = jnp.where(lane == 0, 0.0, n) if j == 0 else n
                m[j, at, :] = n.astype(jnp.bfloat16)
                counts.append(n)
            while len(counts) > 1:
                counts = [a + b for a, b in zip(counts[::2], counts[1::2])]
            acc[at, :] = counts[0].astype(jnp.bfloat16)
        first += part

    sub, lane = positions((8, LANES))
    flat_totals = lax.dot_general(
        jnp.ones((8, LANES), jnp.bfloat16), acc[...], (((1,), (1,)), ((), ())),
        preferred_element_type=jnp.float32,
    )
    row_totals = jnp.zeros((8, LANES), jnp.float32)
    for s in range(8):
        row_totals = jnp.where(sub == s, flat_totals[:, LANES * s : LANES * (s + 1)], row_totals)
    (down,) = running_turns([own_col[...]])
    edge_x[16:24, :] = down + row_totals - col_steps[0, 0, 0].astype(jnp.float32)
    get_bottom.wait()
    get_corner.wait()
    down_total = down[7:8, LANES - 1 : LANES] - row_steps[0, 0, 0].astype(jnp.float32)
    for s in range(8):
        edge_y[5:6, LANES * s : LANES * (s + 1)] = jnp.broadcast_to(down_total, (1, LANES))

    def halo(src_ref, dst_ref, k, device):
        return pltpu.make_async_remote_copy(
            src_ref=src_ref, dst_ref=dst_ref, send_sem=halo_send.at[k], recv_sem=halo_recv.at[k],
            device_id=device, device_id_type=MESH,
        )

    next_row, next_col = lax.rem(r + 1, n_row), lax.rem(c + 1, n_col)
    to_right = halo(edge_x, left, 0, {"col": next_col})
    to_below = halo(edge_y.at[pl.ds(5, 3), :], above.at[pl.ds(5, 3), :], 1, {"row": next_row})
    to_both = halo(bottom, corner, 2, {"row": next_row, "col": next_col})
    sends = ((has_below, to_below), (has_right, to_right), (has_right & has_below, to_both))
    arrivals = ((r > 0, to_below), (c > 0, to_right), ((r > 0) & (c > 0), to_both))

    for holds, copy in sends:
        @pl.when(holds)
        def _(copy=copy):
            copy.start()

    for s in range(8):
        mcol[pl.ds(LANES * s, LANES), :] = jnp.broadcast_to(down[s : s + 1, :], (LANES, LANES)).T
    ta, tb = positions(tri.shape)
    tri[...] = ((ta <= tb) | (tb >= 2 * LANES)).astype(jnp.float32).astype(jnp.bfloat16)

    @pl.loop(0, rows // 256)
    def _(k):
        at = pl.ds(pl.multiple_of(k * 256, 256), 256)
        base = mcol[at, :]
        for j in range(blocks // 2):
            counted = jnp.dot(
                jnp.concatenate([m[2 * j, at, :], m[2 * j + 1, at, :]], axis=1), tri[...],
                preferred_element_type=jnp.float32,
            )
            for h in range(2):
                here = pl.ds(LANES * (2 * j + h), LANES)
                pre[at, here] = x[at, here] * PER_CYCLE - counted[:, LANES * h : LANES * (h + 1)] - base
            base = base + counted[:, 2 * LANES :]

    for holds, copy in arrivals:
        @pl.when(holds)
        def _(copy=copy):
            copy.wait_recv()

    col0, row0 = own_col[...], row_line(x, 0)
    col_in, col_out = left[0:8, :], left[8:16, :]
    row_in, row_out = row_line(above, 6), row_line(above, 7)
    weight_x = edge_weight(
        col_in, col_out, corner[7:8, LANES - 2 : LANES - 1], corner[7:8, LANES - 1 : LANES], r == 0
    )
    weight_y = edge_weight(
        row_in, row_out, corner[6:7, LANES - 1 : LANES], corner[7:8, LANES - 1 : LANES], c == 0
    )
    along, along_above = running_turns([row0, row_out])
    miss_x = down - left[16:24, :] - turns(col0 - col_out)
    miss_y = along - along_above - above[5:6, 0:LANES] - turns(row0 - row_out)
    mean_x = total(weight_x * miss_x) / total(weight_x)
    mean_y = total(weight_y * miss_y) / total(weight_y)
    jump_x[...] = jnp.broadcast_to(jnp.where(c == 0, 0.0, mean_x), (8, LANES))
    jump_y[...] = jnp.broadcast_to(jnp.where(r == 0, 0.0, mean_y), (8, LANES))

    def to_row(t):
        return pltpu.make_async_remote_copy(
            src_ref=jump_y.at[pl.ds(0, 1), :], dst_ref=seen_y.at[pl.ds(r, 1), :],
            send_sem=y_send.at[t], recv_sem=y_recv.at[r],
            device_id={"row": t}, device_id_type=MESH,
        )

    def to_col(t):
        return pltpu.make_async_remote_copy(
            src_ref=jump_x.at[pl.ds(0, 1), :], dst_ref=seen_x.at[pl.ds(c, 1), :],
            send_sem=x_send.at[t], recv_sem=x_recv.at[c],
            device_id={"col": t}, device_id_type=MESH,
        )

    def from_row(k):
        return pltpu.make_async_remote_copy(
            src_ref=jump_y.at[pl.ds(0, 1), :], dst_ref=seen_y.at[pl.ds(k, 1), :],
            send_sem=y_send.at[k], recv_sem=y_recv.at[k],
            device_id={"row": k}, device_id_type=MESH,
        )

    def from_col(k):
        return pltpu.make_async_remote_copy(
            src_ref=jump_x.at[pl.ds(0, 1), :], dst_ref=seen_x.at[pl.ds(k, 1), :],
            send_sem=x_send.at[k], recv_sem=x_recv.at[k],
            device_id={"col": k}, device_id_type=MESH,
        )

    def first_row(t):
        return pltpu.make_async_remote_copy(
            src_ref=jump_y.at[pl.ds(0, 1), :], dst_ref=first_y.at[pl.ds(0, 1), :],
            send_sem=y_send.at[t], recv_sem=first_recv.at[0],
            device_id={"row": t}, device_id_type=MESH,
        )

    def first_col(t):
        return pltpu.make_async_remote_copy(
            src_ref=jump_x.at[pl.ds(0, 1), :], dst_ref=first_x.at[pl.ds(0, 1), :],
            send_sem=x_send.at[t], recv_sem=first_recv.at[1],
            device_id={"col": t}, device_id_type=MESH,
        )

    def send_y(t):
        pl.semaphore_wait(ready_y.at[t], 1)
        to_row(t).start()

    def send_x(t):
        pl.semaphore_wait(ready_x.at[t], 1)
        to_col(t).start()

    stop_x = jnp.where(c < n_col // 4, n_col // 2, n_col)
    start_y, start_x = jnp.where(r == 0, n_row, r + 1), jnp.where(c == 0, stop_x, c + 1)
    near_y, near_x = jnp.minimum(start_y + NEAR, n_row), jnp.minimum(start_x + NEAR, stop_x)
    pl.loop(start_y, near_y)(send_y)
    pl.loop(start_x, near_x)(send_x)
    pl.loop(near_y, n_row)(send_y)
    pl.loop(near_x, stop_x)(send_x)

    @pl.loop(1, r)
    def _(k):
        from_row(k).wait_recv()

    @pl.loop(1, c)
    def _(k):
        from_col(k).wait_recv()

    seen = lax.broadcasted_iota(jnp.int32, (n_col, LANES), 0)
    across = jnp.sum(jnp.where((seen > 0) & (seen < c), seen_x[...], 0.0), axis=0, keepdims=True) + jump_x[0:1, :]
    seen = lax.broadcasted_iota(jnp.int32, (n_row, LANES), 0)
    downs = jnp.sum(jnp.where((seen > 0) & (seen < r), seen_y[...], 0.0), axis=0, keepdims=True) + jump_y[0:1, :]

    @pl.when(r == 0)
    def _():
        jump_y[...] = jnp.broadcast_to(across, (8, LANES))

        @pl.loop(1, n_row)
        def _(t):
            pl.semaphore_wait(ready_y.at[t], 1)
            first_row(t).start()

    @pl.when(c == 0)
    def _():
        jump_x[...] = jnp.broadcast_to(downs, (8, LANES))

        @pl.loop(1, n_col)
        def _(t):
            pl.semaphore_wait(ready_x.at[t], 1)
            first_col(t).start()

    @pl.when(c > 0)
    def _():
        pl.loop(stop_x, n_col)(send_x)

    @pl.when(r > 0)
    def _():
        first_row(0).wait_recv()

    @pl.when(c > 0)
    def _():
        first_col(0).wait_recv()

    across_top = jnp.where(r == 0, across, first_y[0:1, :])
    downs_left = jnp.where(c == 0, downs, first_x[0:1, :])

    mine = top_tile = left_tile = origin = jnp.zeros((1, LANES), jnp.float32)
    for sweep in range(ITERS):
        prefix_across = across + left_tile - mine
        prefix_across_top = across_top + origin - top_tile
        prefix_down = downs + top_tile - mine
        prefix_down_left = downs_left + origin - left_tile
        mine = mine + 0.5 * (prefix_across + prefix_across_top + prefix_down + prefix_down_left)
        top_tile = top_tile + 0.5 * (prefix_across_top + prefix_across_top)
        left_tile = left_tile + 0.5 * (prefix_down_left + prefix_down_left)
    offset[...] = jnp.broadcast_to(mine, (8, LANES))

    for holds, copy in sends:
        @pl.when(holds)
        def _(copy=copy):
            copy.wait_send()

    @pl.loop(r + 1, n_row)
    def _(t):
        to_row(t).wait_send()

    @pl.loop(c + 1, n_col)
    def _(t):
        to_col(t).wait_send()


def add_offset(pre, offset, out, done, sem):
    piece = pre.shape[0] // PIECES
    copies = []
    for k in range(PIECES):
        at = pl.ds(k * piece, piece)
        done[at, :] = pre[at, :] + offset[0:1, 0:1]
        copy = pltpu.make_async_copy(done.at[at, :], out.at[0, at, :], sem.at[k])
        copy.start()
        copies.append(copy)
    for copy in copies:
        copy.wait()


def on_device(n_row, n_col, wrapped, col_steps, row_steps):
    _, rows, cols = wrapped.shape
    f32 = jnp.float32
    line = pltpu.VMEM((8, LANES), f32)
    dma = pltpu.SemaphoreType.DMA
    in_hbm = pl.BlockSpec(memory_space=pltpu.HBM)
    in_smem = pl.BlockSpec(memory_space=pltpu.SMEM)
    in_vmem = pl.BlockSpec(memory_space=pltpu.VMEM)
    pre, offset = pl.pallas_call(
        functools.partial(kernel, n_row, n_col),
        out_shape=(jax.ShapeDtypeStruct((rows, cols), f32), jax.ShapeDtypeStruct((8, LANES), f32)),
        in_specs=[in_hbm, in_smem, in_smem],
        out_specs=(in_vmem, in_vmem),
        scratch_shapes=[
            pltpu.VMEM((rows, cols), f32),
            pltpu.VMEM((cols // LANES, rows, LANES), jnp.bfloat16),
            pltpu.VMEM((rows, LANES), jnp.bfloat16),
            pltpu.VMEM((rows, LANES), f32),
            pltpu.VMEM((2 * LANES, 3 * LANES), jnp.bfloat16),
            line,
            line,
            pltpu.VMEM((24, LANES), f32),
            pltpu.VMEM((8, cols), f32),
            pltpu.VMEM((24, LANES), f32),
            pltpu.VMEM((8, cols), f32),
            line,
            line,
            line,
            pltpu.VMEM((n_col, LANES), f32),
            pltpu.VMEM((n_row, LANES), f32),
            line,
            line,
            dma((len(PARTS),)),
            dma((2,)),
            dma((3,)),
            dma((3,)),
            pltpu.SemaphoreType.REGULAR((n_col,)),
            pltpu.SemaphoreType.REGULAR((n_row,)),
            dma((n_col,)),
            dma((n_col,)),
            dma((n_row,)),
            dma((n_row,)),
            dma((2,)),
        ],
        compiler_params=pltpu.CompilerParams(
            collective_id=0, has_side_effects=True, vmem_limit_bytes=24 * 1024 * 1024
        ),
    )(pltpu.with_memory_space_constraint(wrapped, pltpu.HBM), col_steps, row_steps)
    out = pl.pallas_call(
        add_offset,
        out_shape=jax.ShapeDtypeStruct((1, rows, cols), f32),
        in_specs=[in_vmem, in_vmem],
        out_specs=in_hbm,
        scratch_shapes=[pltpu.VMEM((rows, cols), f32), dma((PIECES,))],
        compiler_params=pltpu.CompilerParams(vmem_limit_bytes=8 * 1024 * 1024),
    )(pre, offset)
    return out


def solution(mesh):
    spec = P(None, "row", "col")
    return jax.shard_map(
        functools.partial(on_device, mesh.shape["row"], mesh.shape["col"]),
        mesh=mesh, in_specs=(spec, spec, spec), out_specs=spec, check_vma=False,
    )
```

```python
import functools
import math

import jax
import jax.numpy as jnp
from jax import lax
from jax.experimental import pallas as pl
from jax.experimental.pallas import tpu as pltpu
from jax.sharding import PartitionSpec as P

ITERS = 2
PER_CYCLE = 1.0 / (2.0 * math.pi)
MESH = pl.DeviceIdType.MESH
LANES = 128
STRIP = 16
PARTS = (256, 256, 256, 256)
MEET = 2
PIECES = 8
NEAR = 3
SIDE = 4


def turns(change):
    return jnp.floor(change * PER_CYCLE + 0.5)


def positions(shape):
    return lax.broadcasted_iota(jnp.int32, shape, 0), lax.broadcasted_iota(jnp.int32, shape, 1)


def before(line, first):
    sub, lane = positions(line.shape)
    along = pltpu.roll(line, 1, 1)
    moved = jnp.where(lane == 0, pltpu.roll(along, 1, 0), along)
    return jnp.where((lane == 0) & (sub == 0), first, moved)


def line_turns(line):
    return turns(line - before(line, line))


def edge_weight(inner, outer, inner_first, outer_first, no_first):
    sub, lane = positions(inner.shape)
    cross = turns(outer - inner)
    cross_before = before(cross, turns(outer_first - inner_first))
    along_inner = turns(inner - before(inner, inner_first))
    along_outer = turns(outer - before(outer, outer_first))
    charge = jnp.abs(cross_before - cross + along_outer - along_inner)
    charge = jnp.where((lane == 0) & (sub == 0) & no_first, 0.0, charge)
    return 1.0 / (1.0 + charge)


def total(x):
    return jnp.sum(jnp.sum(x, axis=1, keepdims=True), axis=0, keepdims=True)


def running_turns(lines):
    stack = jnp.concatenate([line_turns(v) for v in lines], axis=0)
    sub, _ = positions(stack.shape)
    sub = lax.rem(sub, 8)
    carry = jnp.where(sub >= 1, pltpu.roll(stack, 1, 0), 0.0)
    for step in (1, 2, 4):
        carry = carry + jnp.where(sub >= step, pltpu.roll(carry, step, 0), 0.0)
    ka, kb = positions((2 * LANES, LANES))
    prefix = jnp.dot(
        jnp.concatenate([stack, carry], axis=1).astype(jnp.bfloat16),
        ((ka <= kb) | (ka >= LANES)).astype(jnp.float32).astype(jnp.bfloat16),
        preferred_element_type=jnp.float32,
    )
    return [prefix[8 * k : 8 * k + 8] for k in range(len(lines))]


def row_line(ref, i):
    return jnp.concatenate([ref[i : i + 1, LANES * s : LANES * (s + 1)] for s in range(8)], axis=0)


def far_side(low, high):
    def level(t):
        return jnp.minimum(lax.div(t, SIDE), SIDE // 2) + jnp.minimum(lax.rem(t, SIDE), SIDE // 2)

    return level(high) >= level(low)


def kernel(
    n_row, n_col, wrapped, col_steps, row_steps, pre, offset,
    x, sides, m, acc, mcol, tri, own_col, bottom, edge_x, edge_y, left, above, corner,
    jump_x, jump_y, seen_x, seen_y, first_x, first_y,
    in_sem, edge_sem, halo_send, halo_recv, ready_x, ready_y, x_send, x_recv, y_send, y_recv, first_recv,
):
    r, c = lax.axis_index("row"), lax.axis_index("col")
    rows, cols = x.shape
    blocks = cols // LANES
    src = wrapped.at[0]

    get_bottom = pltpu.make_async_copy(src.at[pl.ds(rows - 8, 8), :], edge_y, edge_sem.at[0])
    get_corner = pltpu.make_async_copy(
        src.at[pl.ds(rows - 8, 8), pl.ds(cols - LANES, LANES)], bottom, edge_sem.at[1]
    )
    get_parts = [
        pltpu.make_async_copy(
            src.at[pl.ds(sum(PARTS[:k]), part), :], x.at[pl.ds(sum(PARTS[:k]), part), :], in_sem.at[k]
        )
        for k, part in enumerate(PARTS)
    ]
    get_sides = [
        pltpu.make_async_copy(src.at[:, pl.ds(at, LANES)], sides.at[k], edge_sem.at[2 + k])
        for k, at in enumerate((0, cols - LANES))
    ]
    for copy in [get_sides[0]] + get_parts[:MEET] + [get_bottom, get_corner] + get_parts[MEET:] + [get_sides[1]]:
        copy.start()

    barrier = pltpu.get_barrier_semaphore()

    def greet(device):
        pl.semaphore_signal(barrier, inc=1, device_id=device, device_id_type=MESH)

    @pl.when(c > 0)
    def _():
        greet({"col": c - 1})

    @pl.when((r > 0) & (c > 0))
    def _():
        greet({"row": r - 1, "col": c - 1})

    @pl.loop(0, r)
    def _(k):
        at = r - 1 - k

        @pl.when((k == 0) | jnp.logical_not(far_side(at, r)))
        def _():
            greet({"row": at})

    @pl.loop(r + 1, n_row)
    def _(t):
        @pl.when(far_side(r, t))
        def _():
            greet({"row": t})

    @pl.loop(c + 1, n_col)
    def _(t):
        greet({"col": t})

    has_right, has_below = c < n_col - 1, r < n_row - 1
    expected = c + has_right.astype(jnp.int32) + (has_right & has_below).astype(jnp.int32)
    for k in range(n_row):
        from_low = (k < r) & far_side(k, r)
        from_high = (k == r + 1) | ((k > r) & jnp.logical_not(far_side(r, k)))
        expected = expected + (from_low | from_high).astype(jnp.int32)

    def meet():
        get_bottom.wait()
        get_corner.wait()
        down_total = down[7:8, LANES - 1 : LANES] - row_steps[0, 0, 0].astype(jnp.float32)
        for s in range(8):
            edge_y[5:6, LANES * s : LANES * (s + 1)] = jnp.broadcast_to(down_total, (1, LANES))
        pl.semaphore_wait(barrier, expected)

        @pl.when(has_below)
        def _():
            to_below.start()

        @pl.when(has_right & has_below)
        def _():
            to_both.start()

        @pl.loop(1, r)
        def _(k):
            at = r - 1 - k

            @pl.when(far_side(at, r))
            def _():
                pl.semaphore_signal(ready_y.at[r], inc=1, device_id={"row": at}, device_id_type=MESH)

        @pl.loop(1, c)
        def _(k):
            pl.semaphore_signal(
                ready_x.at[c], inc=1, device_id={"col": c - 1 - k}, device_id_type=MESH
            )

    get_sides[0].wait()
    for s in range(8):
        own_col[pl.ds(s, 1), :] = sides[0, pl.ds(LANES * s, LANES), :].T[0:1, :]
    (down,) = running_turns([own_col[...]])
    def halo(src_ref, dst_ref, k, device):
        return pltpu.make_async_remote_copy(
            src_ref=src_ref, dst_ref=dst_ref, send_sem=halo_send.at[k], recv_sem=halo_recv.at[k],
            device_id=device, device_id_type=MESH,
        )

    next_row, next_col = lax.rem(r + 1, n_row), lax.rem(c + 1, n_col)
    to_right = halo(edge_x, left, 0, {"col": next_col})
    to_below = halo(edge_y.at[pl.ds(5, 3), :], above.at[pl.ds(5, 3), :], 1, {"row": next_row})
    to_both = halo(bottom, corner, 2, {"row": next_row, "col": next_col})
    sends = ((has_below, to_below), (has_right, to_right), (has_right & has_below, to_both))
    arrivals = ((r > 0, to_below), (c > 0, to_right), ((r > 0) & (c > 0), to_both))

    first = 0
    for k, part in enumerate(PARTS):
        if k == MEET:
            meet()
        get_parts[k].wait()
        for q in range(first // STRIP, (first + part) // STRIP):
            at = pl.ds(STRIP * q, STRIP)
            lane = lax.broadcasted_iota(jnp.int32, (STRIP, LANES), 1)
            counts, moved = [], None
            for j in range(blocks):
                here = x[at, pl.ds(LANES * j, LANES)]
                last, moved = moved, pltpu.roll(here, 1, 1)
                back = moved if j == 0 else jnp.where(lane == 0, last, moved)
                n = turns(here - back)
                n = jnp.where(lane == 0, 0.0, n) if j == 0 else n
                m[j, at, :] = n.astype(jnp.bfloat16)
                counts.append(n)
            while len(counts) > 1:
                counts = [a + b for a, b in zip(counts[::2], counts[1::2])]
            acc[at, :] = counts[0].astype(jnp.bfloat16)
        first += part

    get_sides[1].wait()
    for s in range(8):
        turned = sides[1, pl.ds(LANES * s, LANES), :].T
        edge_x[pl.ds(s, 1), :] = turned[LANES - 2 : LANES - 1, :]
        edge_x[pl.ds(8 + s, 1), :] = turned[LANES - 1 : LANES, :]

    sub, lane = positions((8, LANES))
    flat_totals = lax.dot_general(
        jnp.ones((8, LANES), jnp.bfloat16), acc[...], (((1,), (1,)), ((), ())),
        preferred_element_type=jnp.float32,
    )
    row_totals = jnp.zeros((8, LANES), jnp.float32)
    for s in range(8):
        row_totals = jnp.where(sub == s, flat_totals[:, LANES * s : LANES * (s + 1)], row_totals)
    edge_x[16:24, :] = down + row_totals - col_steps[0, 0, 0].astype(jnp.float32)
    @pl.when(has_right)
    def _():
        to_right.start()

    for holds, copy in arrivals:
        @pl.when(holds)
        def _(copy=copy):
            copy.wait_recv()

    col0, row0 = own_col[...], row_line(x, 0)
    col_in, col_out = left[0:8, :], left[8:16, :]
    row_in, row_out = row_line(above, 6), row_line(above, 7)
    weight_x = edge_weight(
        col_in, col_out, corner[7:8, LANES - 2 : LANES - 1], corner[7:8, LANES - 1 : LANES], r == 0
    )
    weight_y = edge_weight(
        row_in, row_out, corner[6:7, LANES - 1 : LANES], corner[7:8, LANES - 1 : LANES], c == 0
    )
    along, along_above = running_turns([row0, row_out])
    miss_x = down - left[16:24, :] - turns(col0 - col_out)
    miss_y = along - along_above - above[5:6, 0:LANES] - turns(row0 - row_out)
    mean_x = total(weight_x * miss_x) / total(weight_x)
    mean_y = total(weight_y * miss_y) / total(weight_y)
    jump_x[...] = jnp.broadcast_to(jnp.where(c == 0, 0.0, mean_x), (8, LANES))
    jump_y[...] = jnp.broadcast_to(jnp.where(r == 0, 0.0, mean_y), (8, LANES))

    def to_row(t):
        return pltpu.make_async_remote_copy(
            src_ref=jump_y.at[pl.ds(0, 1), :], dst_ref=seen_y.at[pl.ds(r, 1), :],
            send_sem=y_send.at[t], recv_sem=y_recv.at[r],
            device_id={"row": t}, device_id_type=MESH,
        )

    def to_col(t):
        return pltpu.make_async_remote_copy(
            src_ref=jump_x.at[pl.ds(0, 1), :], dst_ref=seen_x.at[pl.ds(c, 1), :],
            send_sem=x_send.at[t], recv_sem=x_recv.at[c],
            device_id={"col": t}, device_id_type=MESH,
        )

    def from_row(k):
        return pltpu.make_async_remote_copy(
            src_ref=jump_y.at[pl.ds(0, 1), :], dst_ref=seen_y.at[pl.ds(k, 1), :],
            send_sem=y_send.at[k], recv_sem=y_recv.at[k],
            device_id={"row": k}, device_id_type=MESH,
        )

    def from_col(k):
        return pltpu.make_async_remote_copy(
            src_ref=jump_x.at[pl.ds(0, 1), :], dst_ref=seen_x.at[pl.ds(k, 1), :],
            send_sem=x_send.at[k], recv_sem=x_recv.at[k],
            device_id={"col": k}, device_id_type=MESH,
        )

    def first_row(t):
        return pltpu.make_async_remote_copy(
            src_ref=jump_y.at[pl.ds(0, 1), :], dst_ref=first_y.at[pl.ds(0, 1), :],
            send_sem=y_send.at[t], recv_sem=first_recv.at[0],
            device_id={"row": t}, device_id_type=MESH,
        )

    def first_col(t):
        return pltpu.make_async_remote_copy(
            src_ref=jump_x.at[pl.ds(0, 1), :], dst_ref=first_x.at[pl.ds(0, 1), :],
            send_sem=x_send.at[t], recv_sem=first_recv.at[1],
            device_id={"col": t}, device_id_type=MESH,
        )

    def await_y(t):
        @pl.when((t > r + 1) & far_side(r, t))
        def _():
            pl.semaphore_wait(ready_y.at[t], 1)

    def await_x(t):
        @pl.when(t > c + 1)
        def _():
            pl.semaphore_wait(ready_x.at[t], 1)

    def send_y(t):
        await_y(t)
        to_row(t).start()

    def send_x(t):
        await_x(t)
        to_col(t).start()

    stop_x = jnp.where(c < n_col // 4, n_col // 2, n_col)
    start_y, start_x = jnp.where(r == 0, n_row, r + 1), jnp.where(c == 0, stop_x, c + 1)
    near_y, near_x = jnp.minimum(start_y + NEAR, n_row), jnp.minimum(start_x + NEAR, stop_x)
    pl.loop(start_y, near_y)(send_y)
    pl.loop(start_x, near_x)(send_x)
    late_x = jnp.where(c < n_col // 2, near_x, stop_x)
    pl.loop(near_x, late_x)(send_x)
    pl.loop(near_y, n_row)(send_y)
    pl.loop(late_x, stop_x)(send_x)

    for s in range(8):
        mcol[pl.ds(LANES * s, LANES), :] = jnp.broadcast_to(down[s : s + 1, :], (LANES, LANES)).T
    ta, tb = positions(tri.shape)
    tri[...] = ((ta <= tb) | (tb >= 2 * LANES)).astype(jnp.float32).astype(jnp.bfloat16)

    @pl.loop(0, rows // 256)
    def _(k):
        at = pl.ds(pl.multiple_of(k * 256, 256), 256)
        base = mcol[at, :]
        for j in range(blocks // 2):
            counted = jnp.dot(
                jnp.concatenate([m[2 * j, at, :], m[2 * j + 1, at, :]], axis=1), tri[...],
                preferred_element_type=jnp.float32,
            )
            for h in range(2):
                here = pl.ds(LANES * (2 * j + h), LANES)
                pre[at, here] = x[at, here] * PER_CYCLE - counted[:, LANES * h : LANES * (h + 1)] - base
            base = base + counted[:, 2 * LANES :]

    @pl.loop(1, r)
    def _(k):
        from_row(k).wait_recv()

    @pl.loop(1, c)
    def _(k):
        from_col(k).wait_recv()

    seen = lax.broadcasted_iota(jnp.int32, (n_col, LANES), 0)
    across = jnp.sum(jnp.where((seen > 0) & (seen < c), seen_x[...], 0.0), axis=0, keepdims=True) + jump_x[0:1, :]
    seen = lax.broadcasted_iota(jnp.int32, (n_row, LANES), 0)
    downs = jnp.sum(jnp.where((seen > 0) & (seen < r), seen_y[...], 0.0), axis=0, keepdims=True) + jump_y[0:1, :]

    @pl.when(r == 0)
    def _():
        jump_y[...] = jnp.broadcast_to(across, (8, LANES))

        @pl.loop(1, n_row)
        def _(t):
            await_y(t)
            first_row(t).start()

    @pl.when(c == 0)
    def _():
        jump_x[...] = jnp.broadcast_to(downs, (8, LANES))

        @pl.loop(1, n_col)
        def _(t):
            await_x(t)
            first_col(t).start()

    @pl.when(c > 0)
    def _():
        pl.loop(stop_x, n_col)(send_x)

    @pl.when(r > 0)
    def _():
        first_row(0).wait_recv()

    @pl.when(c > 0)
    def _():
        first_col(0).wait_recv()

    across_top = jnp.where(r == 0, across, first_y[0:1, :])
    downs_left = jnp.where(c == 0, downs, first_x[0:1, :])

    mine = top_tile = left_tile = origin = jnp.zeros((1, LANES), jnp.float32)
    for sweep in range(ITERS):
        prefix_across = across + left_tile - mine
        prefix_across_top = across_top + origin - top_tile
        prefix_down = downs + top_tile - mine
        prefix_down_left = downs_left + origin - left_tile
        mine = mine + 0.5 * (prefix_across + prefix_across_top + prefix_down + prefix_down_left)
        top_tile = top_tile + 0.5 * (prefix_across_top + prefix_across_top)
        left_tile = left_tile + 0.5 * (prefix_down_left + prefix_down_left)
    offset[...] = jnp.broadcast_to(mine, (8, LANES))

    for holds, copy in sends:
        @pl.when(holds)
        def _(copy=copy):
            copy.wait_send()

    @pl.loop(r + 1, n_row)
    def _(t):
        to_row(t).wait_send()

    @pl.loop(c + 1, n_col)
    def _(t):
        to_col(t).wait_send()


def add_offset(pre, offset, out, done, sem):
    piece = pre.shape[0] // PIECES
    copies = []
    for k in range(PIECES):
        at = pl.ds(k * piece, piece)
        done[at, :] = pre[at, :] + offset[0:1, 0:1]
        copy = pltpu.make_async_copy(done.at[at, :], out.at[0, at, :], sem.at[k])
        copy.start()
        copies.append(copy)
    for copy in copies:
        copy.wait()


def on_device(n_row, n_col, wrapped, col_steps, row_steps):
    _, rows, cols = wrapped.shape
    f32 = jnp.float32
    line = pltpu.VMEM((8, LANES), f32)
    dma = pltpu.SemaphoreType.DMA
    in_hbm = pl.BlockSpec(memory_space=pltpu.HBM)
    in_smem = pl.BlockSpec(memory_space=pltpu.SMEM)
    in_vmem = pl.BlockSpec(memory_space=pltpu.VMEM)
    pre, offset = pl.pallas_call(
        functools.partial(kernel, n_row, n_col),
        out_shape=(jax.ShapeDtypeStruct((rows, cols), f32), jax.ShapeDtypeStruct((8, LANES), f32)),
        in_specs=[in_hbm, in_smem, in_smem],
        out_specs=(in_vmem, in_vmem),
        scratch_shapes=[
            pltpu.VMEM((rows, cols), f32),
            pltpu.VMEM((2, rows, LANES), f32),
            pltpu.VMEM((cols // LANES, rows, LANES), jnp.bfloat16),
            pltpu.VMEM((rows, LANES), jnp.bfloat16),
            pltpu.VMEM((rows, LANES), f32),
            pltpu.VMEM((2 * LANES, 3 * LANES), jnp.bfloat16),
            line,
            line,
            pltpu.VMEM((24, LANES), f32),
            pltpu.VMEM((8, cols), f32),
            pltpu.VMEM((24, LANES), f32),
            pltpu.VMEM((8, cols), f32),
            line,
            line,
            line,
            pltpu.VMEM((n_col, LANES), f32),
            pltpu.VMEM((n_row, LANES), f32),
            line,
            line,
            dma((len(PARTS),)),
            dma((4,)),
            dma((3,)),
            dma((3,)),
            pltpu.SemaphoreType.REGULAR((n_col,)),
            pltpu.SemaphoreType.REGULAR((n_row,)),
            dma((n_col,)),
            dma((n_col,)),
            dma((n_row,)),
            dma((n_row,)),
            dma((2,)),
        ],
        compiler_params=pltpu.CompilerParams(
            collective_id=0, has_side_effects=True, vmem_limit_bytes=24 * 1024 * 1024
        ),
    )(pltpu.with_memory_space_constraint(wrapped, pltpu.HBM), col_steps, row_steps)
    out = pl.pallas_call(
        add_offset,
        out_shape=jax.ShapeDtypeStruct((1, rows, cols), f32),
        in_specs=[in_vmem, in_vmem],
        out_specs=in_hbm,
        scratch_shapes=[pltpu.VMEM((rows, cols), f32), dma((PIECES,))],
        compiler_params=pltpu.CompilerParams(vmem_limit_bytes=8 * 1024 * 1024),
    )(pre, offset)
    return out


def solution(mesh):
    spec = P(None, "row", "col")
    return jax.shard_map(
        functools.partial(on_device, mesh.shape["row"], mesh.shape["col"]),
        mesh=mesh, in_specs=(spec, spec, spec), out_specs=spec, check_vma=False,
    )
```

```python
import functools
import math

import jax
import jax.numpy as jnp
from jax import lax
from jax.experimental import pallas as pl
from jax.experimental.pallas import tpu as pltpu
from jax.sharding import PartitionSpec as P

ITERS = 2
PER_CYCLE = 1.0 / (2.0 * math.pi)
MESH = pl.DeviceIdType.MESH
LANES = 128
STRIP = 16
PARTS = (256, 256, 256, 256)
MEET = 2
PIECES = 8
NEAR = 3
SIDE = 4


def turns(change):
    return jnp.floor(change * PER_CYCLE + 0.5)


def positions(shape):
    return lax.broadcasted_iota(jnp.int32, shape, 0), lax.broadcasted_iota(jnp.int32, shape, 1)


def before(line, first):
    sub, lane = positions(line.shape)
    along = pltpu.roll(line, 1, 1)
    moved = jnp.where(lane == 0, pltpu.roll(along, 1, 0), along)
    return jnp.where((lane == 0) & (sub == 0), first, moved)


def line_turns(line):
    return turns(line - before(line, line))


def edge_weight(inner, outer, inner_first, outer_first, no_first):
    sub, lane = positions(inner.shape)
    cross = turns(outer - inner)
    cross_before = before(cross, turns(outer_first - inner_first))
    along_inner = turns(inner - before(inner, inner_first))
    along_outer = turns(outer - before(outer, outer_first))
    charge = jnp.abs(cross_before - cross + along_outer - along_inner)
    charge = jnp.where((lane == 0) & (sub == 0) & no_first, 0.0, charge)
    return 1.0 / (1.0 + charge)


def total(x):
    return jnp.sum(jnp.sum(x, axis=1, keepdims=True), axis=0, keepdims=True)


def running_turns(lines):
    stack = jnp.concatenate([line_turns(v) for v in lines], axis=0)
    sub, _ = positions(stack.shape)
    sub = lax.rem(sub, 8)
    carry = jnp.where(sub >= 1, pltpu.roll(stack, 1, 0), 0.0)
    for step in (1, 2, 4):
        carry = carry + jnp.where(sub >= step, pltpu.roll(carry, step, 0), 0.0)
    ka, kb = positions((2 * LANES, LANES))
    prefix = jnp.dot(
        jnp.concatenate([stack, carry], axis=1).astype(jnp.bfloat16),
        ((ka <= kb) | (ka >= LANES)).astype(jnp.float32).astype(jnp.bfloat16),
        preferred_element_type=jnp.float32,
    )
    return [prefix[8 * k : 8 * k + 8] for k in range(len(lines))]


def row_line(ref, i):
    return jnp.concatenate([ref[i : i + 1, LANES * s : LANES * (s + 1)] for s in range(8)], axis=0)


def distance(t):
    return jnp.minimum(lax.div(t, SIDE), SIDE // 2) + jnp.minimum(lax.rem(t, SIDE), SIDE // 2)


def kernel(
    n_row, n_col, wrapped, col_steps, row_steps, pre, offset,
    x, sides, m, acc, mcol, tri, own_col, bottom, edge_x, edge_y, left, above, corner,
    jump_x, jump_y, seen_x, seen_y, first_x, first_y,
    in_sem, edge_sem, halo_send, halo_recv, ready_x, ready_y, x_send, x_recv, y_send, y_recv, first_recv,
):
    r, c = lax.axis_index("row"), lax.axis_index("col")
    rows, cols = x.shape
    blocks = cols // LANES
    src = wrapped.at[0]

    get_bottom = pltpu.make_async_copy(src.at[pl.ds(rows - 8, 8), :], edge_y, edge_sem.at[0])
    get_corner = pltpu.make_async_copy(
        src.at[pl.ds(rows - 8, 8), pl.ds(cols - LANES, LANES)], bottom, edge_sem.at[1]
    )
    get_parts = [
        pltpu.make_async_copy(
            src.at[pl.ds(sum(PARTS[:k]), part), :], x.at[pl.ds(sum(PARTS[:k]), part), :], in_sem.at[k]
        )
        for k, part in enumerate(PARTS)
    ]
    get_sides = [
        pltpu.make_async_copy(src.at[:, pl.ds(at, LANES)], sides.at[k], edge_sem.at[2 + k])
        for k, at in enumerate((0, cols - LANES))
    ]
    for copy in [get_sides[0]] + get_parts[:MEET] + [get_bottom, get_corner] + get_parts[MEET:] + [get_sides[1]]:
        copy.start()

    barrier = pltpu.get_barrier_semaphore()

    def greet(device):
        pl.semaphore_signal(barrier, inc=1, device_id=device, device_id_type=MESH)

    away = distance(r)
    row_distance = [min(t // SIDE, SIDE // 2) + min(t % SIDE, SIDE // 2) for t in range(n_row)]
    from_low = [(t < r) & (row_distance[t] <= away) for t in range(n_row)]

    @pl.when(c > 0)
    def _():
        greet({"col": c - 1})

    @pl.when((r > 0) & (c > 0))
    def _():
        greet({"row": r - 1, "col": c - 1})

    for t in range(n_row):
        greets_low = (t < r) & ((t == r - 1) | (row_distance[t] > away))

        @pl.when(greets_low | ((t > r) & (row_distance[t] >= away)))
        def _(t=t):
            greet({"row": t})

    @pl.loop(c + 1, n_col)
    def _(t):
        greet({"col": t})

    has_right, has_below = c < n_col - 1, r < n_row - 1
    expected = c + has_right.astype(jnp.int32) + (has_right & has_below).astype(jnp.int32)
    for t in range(n_row):
        from_high = (t == r + 1) | ((t > r) & (row_distance[t] < away))
        expected = expected + (from_low[t] | from_high).astype(jnp.int32)

    def meet():
        get_bottom.wait()
        get_corner.wait()
        down_total = down[7:8, LANES - 1 : LANES] - row_steps[0, 0, 0].astype(jnp.float32)
        for s in range(8):
            edge_y[5:6, LANES * s : LANES * (s + 1)] = jnp.broadcast_to(down_total, (1, LANES))
        pl.semaphore_wait(barrier, expected)

        @pl.when(has_below)
        def _():
            to_below.start()

        @pl.when(has_right & has_below)
        def _():
            to_both.start()

        for t in reversed(range(n_row)):
            @pl.when(from_low[t] & (t != r - 1))
            def _(t=t):
                pl.semaphore_signal(ready_y.at[r], inc=1, device_id={"row": t}, device_id_type=MESH)

        @pl.loop(1, c)
        def _(k):
            pl.semaphore_signal(
                ready_x.at[c], inc=1, device_id={"col": c - 1 - k}, device_id_type=MESH
            )

    get_sides[0].wait()
    for s in range(8):
        own_col[pl.ds(s, 1), :] = sides[0, pl.ds(LANES * s, LANES), :].T[0:1, :]
    (down,) = running_turns([own_col[...]])
    def halo(src_ref, dst_ref, k, device):
        return pltpu.make_async_remote_copy(
            src_ref=src_ref, dst_ref=dst_ref, send_sem=halo_send.at[k], recv_sem=halo_recv.at[k],
            device_id=device, device_id_type=MESH,
        )

    next_row, next_col = lax.rem(r + 1, n_row), lax.rem(c + 1, n_col)
    to_right = halo(edge_x, left, 0, {"col": next_col})
    to_below = halo(edge_y.at[pl.ds(5, 3), :], above.at[pl.ds(5, 3), :], 1, {"row": next_row})
    to_both = halo(bottom, corner, 2, {"row": next_row, "col": next_col})
    sends = ((has_below, to_below), (has_right, to_right), (has_right & has_below, to_both))
    arrivals = ((r > 0, to_below), (c > 0, to_right), ((r > 0) & (c > 0), to_both))

    first = 0
    for k, part in enumerate(PARTS):
        if k == MEET:
            meet()
        get_parts[k].wait()
        for q in range(first // STRIP, (first + part) // STRIP):
            at = pl.ds(STRIP * q, STRIP)
            lane = lax.broadcasted_iota(jnp.int32, (STRIP, LANES), 1)
            counts, moved = [], None
            for j in range(blocks):
                here = x[at, pl.ds(LANES * j, LANES)]
                last, moved = moved, pltpu.roll(here, 1, 1)
                back = moved if j == 0 else jnp.where(lane == 0, last, moved)
                n = turns(here - back)
                n = jnp.where(lane == 0, 0.0, n) if j == 0 else n
                m[j, at, :] = n.astype(jnp.bfloat16)
                counts.append(n)
            while len(counts) > 1:
                counts = [a + b for a, b in zip(counts[::2], counts[1::2])]
            acc[at, :] = counts[0].astype(jnp.bfloat16)
        first += part

    get_sides[1].wait()
    for s in range(8):
        turned = sides[1, pl.ds(LANES * s, LANES), :].T
        edge_x[pl.ds(s, 1), :] = turned[LANES - 2 : LANES - 1, :]
        edge_x[pl.ds(8 + s, 1), :] = turned[LANES - 1 : LANES, :]

    sub, lane = positions((8, LANES))
    flat_totals = lax.dot_general(
        jnp.ones((8, LANES), jnp.bfloat16), acc[...], (((1,), (1,)), ((), ())),
        preferred_element_type=jnp.float32,
    )
    row_totals = jnp.zeros((8, LANES), jnp.float32)
    for s in range(8):
        row_totals = jnp.where(sub == s, flat_totals[:, LANES * s : LANES * (s + 1)], row_totals)
    edge_x[16:24, :] = down + row_totals - col_steps[0, 0, 0].astype(jnp.float32)
    @pl.when(has_right)
    def _():
        to_right.start()

    for holds, copy in arrivals:
        @pl.when(holds)
        def _(copy=copy):
            copy.wait_recv()

    col0, row0 = own_col[...], row_line(x, 0)
    col_in, col_out = left[0:8, :], left[8:16, :]
    row_in, row_out = row_line(above, 6), row_line(above, 7)
    weight_x = edge_weight(
        col_in, col_out, corner[7:8, LANES - 2 : LANES - 1], corner[7:8, LANES - 1 : LANES], r == 0
    )
    weight_y = edge_weight(
        row_in, row_out, corner[6:7, LANES - 1 : LANES], corner[7:8, LANES - 1 : LANES], c == 0
    )
    along, along_above = running_turns([row0, row_out])
    miss_x = down - left[16:24, :] - turns(col0 - col_out)
    miss_y = along - along_above - above[5:6, 0:LANES] - turns(row0 - row_out)
    mean_x = total(weight_x * miss_x) / total(weight_x)
    mean_y = total(weight_y * miss_y) / total(weight_y)
    jump_x[...] = jnp.broadcast_to(jnp.where(c == 0, 0.0, mean_x), (8, LANES))
    jump_y[...] = jnp.broadcast_to(jnp.where(r == 0, 0.0, mean_y), (8, LANES))

    def to_row(t):
        return pltpu.make_async_remote_copy(
            src_ref=jump_y.at[pl.ds(0, 1), :], dst_ref=seen_y.at[pl.ds(r, 1), :],
            send_sem=y_send.at[t], recv_sem=y_recv.at[r],
            device_id={"row": t}, device_id_type=MESH,
        )

    def to_col(t):
        return pltpu.make_async_remote_copy(
            src_ref=jump_x.at[pl.ds(0, 1), :], dst_ref=seen_x.at[pl.ds(c, 1), :],
            send_sem=x_send.at[t], recv_sem=x_recv.at[c],
            device_id={"col": t}, device_id_type=MESH,
        )

    def from_row(k):
        return pltpu.make_async_remote_copy(
            src_ref=jump_y.at[pl.ds(0, 1), :], dst_ref=seen_y.at[pl.ds(k, 1), :],
            send_sem=y_send.at[k], recv_sem=y_recv.at[k],
            device_id={"row": k}, device_id_type=MESH,
        )

    def from_col(k):
        return pltpu.make_async_remote_copy(
            src_ref=jump_x.at[pl.ds(0, 1), :], dst_ref=seen_x.at[pl.ds(k, 1), :],
            send_sem=x_send.at[k], recv_sem=x_recv.at[k],
            device_id={"col": k}, device_id_type=MESH,
        )

    def first_row(t):
        return pltpu.make_async_remote_copy(
            src_ref=jump_y.at[pl.ds(0, 1), :], dst_ref=first_y.at[pl.ds(0, 1), :],
            send_sem=y_send.at[t], recv_sem=first_recv.at[0],
            device_id={"row": t}, device_id_type=MESH,
        )

    def first_col(t):
        return pltpu.make_async_remote_copy(
            src_ref=jump_x.at[pl.ds(0, 1), :], dst_ref=first_x.at[pl.ds(0, 1), :],
            send_sem=x_send.at[t], recv_sem=first_recv.at[1],
            device_id={"col": t}, device_id_type=MESH,
        )

    def await_y(t):
        @pl.when((t > r + 1) & (away <= distance(t)))
        def _():
            pl.semaphore_wait(ready_y.at[t], 1)

    def await_x(t):
        @pl.when(t > c + 1)
        def _():
            pl.semaphore_wait(ready_x.at[t], 1)

    def send_y(t):
        await_y(t)
        to_row(t).start()

    def send_x(t):
        await_x(t)
        to_col(t).start()

    stop_x = jnp.where(c < n_col // 4, n_col // 2, n_col)
    start_y, start_x = jnp.where(r == 0, n_row, r + 1), jnp.where(c == 0, stop_x, c + 1)
    near_y, near_x = jnp.minimum(start_y + NEAR, n_row), jnp.minimum(start_x + NEAR, stop_x)
    pl.loop(start_y, near_y)(send_y)
    pl.loop(start_x, near_x)(send_x)
    late_x = jnp.where(c < n_col // 2, near_x, stop_x)
    pl.loop(near_x, late_x)(send_x)
    pl.loop(near_y, n_row)(send_y)
    pl.loop(late_x, stop_x)(send_x)

    for s in range(8):
        mcol[pl.ds(LANES * s, LANES), :] = jnp.broadcast_to(down[s : s + 1, :], (LANES, LANES)).T
    ta, tb = positions(tri.shape)
    tri[...] = ((ta <= tb) | (tb >= 2 * LANES)).astype(jnp.float32).astype(jnp.bfloat16)

    @pl.loop(0, rows // 256)
    def _(k):
        at = pl.ds(pl.multiple_of(k * 256, 256), 256)
        base = mcol[at, :]
        for j in range(blocks // 2):
            counted = jnp.dot(
                jnp.concatenate([m[2 * j, at, :], m[2 * j + 1, at, :]], axis=1), tri[...],
                preferred_element_type=jnp.float32,
            )
            for h in range(2):
                here = pl.ds(LANES * (2 * j + h), LANES)
                pre[at, here] = x[at, here] * PER_CYCLE - counted[:, LANES * h : LANES * (h + 1)] - base
            base = base + counted[:, 2 * LANES :]

    @pl.loop(1, r)
    def _(k):
        from_row(k).wait_recv()

    @pl.loop(1, c)
    def _(k):
        from_col(k).wait_recv()

    seen = lax.broadcasted_iota(jnp.int32, (n_col, LANES), 0)
    across = jnp.sum(jnp.where((seen > 0) & (seen < c), seen_x[...], 0.0), axis=0, keepdims=True) + jump_x[0:1, :]
    seen = lax.broadcasted_iota(jnp.int32, (n_row, LANES), 0)
    downs = jnp.sum(jnp.where((seen > 0) & (seen < r), seen_y[...], 0.0), axis=0, keepdims=True) + jump_y[0:1, :]

    @pl.when(r == 0)
    def _():
        jump_y[...] = jnp.broadcast_to(across, (8, LANES))

        @pl.loop(1, n_row)
        def _(t):
            await_y(t)
            first_row(t).start()

    @pl.when(c == 0)
    def _():
        jump_x[...] = jnp.broadcast_to(downs, (8, LANES))

        @pl.loop(1, n_col)
        def _(t):
            await_x(t)
            first_col(t).start()

    @pl.when(c > 0)
    def _():
        pl.loop(stop_x, n_col)(send_x)

    @pl.when(r > 0)
    def _():
        first_row(0).wait_recv()

    @pl.when(c > 0)
    def _():
        first_col(0).wait_recv()

    across_top = jnp.where(r == 0, across, first_y[0:1, :])
    downs_left = jnp.where(c == 0, downs, first_x[0:1, :])

    mine = top_tile = left_tile = origin = jnp.zeros((1, LANES), jnp.float32)
    for sweep in range(ITERS):
        prefix_across = across + left_tile - mine
        prefix_across_top = across_top + origin - top_tile
        prefix_down = downs + top_tile - mine
        prefix_down_left = downs_left + origin - left_tile
        mine = mine + 0.5 * (prefix_across + prefix_across_top + prefix_down + prefix_down_left)
        top_tile = top_tile + 0.5 * (prefix_across_top + prefix_across_top)
        left_tile = left_tile + 0.5 * (prefix_down_left + prefix_down_left)
    offset[...] = jnp.broadcast_to(mine, (8, LANES))

    for holds, copy in sends:
        @pl.when(holds)
        def _(copy=copy):
            copy.wait_send()

    @pl.loop(r + 1, n_row)
    def _(t):
        to_row(t).wait_send()

    @pl.loop(c + 1, n_col)
    def _(t):
        to_col(t).wait_send()


def add_offset(pre, offset, out, done, sem):
    piece = pre.shape[0] // PIECES
    copies = []
    for k in range(PIECES):
        at = pl.ds(k * piece, piece)
        done[at, :] = pre[at, :] + offset[0:1, 0:1]
        copy = pltpu.make_async_copy(done.at[at, :], out.at[0, at, :], sem.at[k])
        copy.start()
        copies.append(copy)
    for copy in copies:
        copy.wait()


def on_device(n_row, n_col, wrapped, col_steps, row_steps):
    _, rows, cols = wrapped.shape
    f32 = jnp.float32
    line = pltpu.VMEM((8, LANES), f32)
    dma = pltpu.SemaphoreType.DMA
    in_hbm = pl.BlockSpec(memory_space=pltpu.HBM)
    in_smem = pl.BlockSpec(memory_space=pltpu.SMEM)
    in_vmem = pl.BlockSpec(memory_space=pltpu.VMEM)
    pre, offset = pl.pallas_call(
        functools.partial(kernel, n_row, n_col),
        out_shape=(jax.ShapeDtypeStruct((rows, cols), f32), jax.ShapeDtypeStruct((8, LANES), f32)),
        in_specs=[in_hbm, in_smem, in_smem],
        out_specs=(in_vmem, in_vmem),
        scratch_shapes=[
            pltpu.VMEM((rows, cols), f32),
            pltpu.VMEM((2, rows, LANES), f32),
            pltpu.VMEM((cols // LANES, rows, LANES), jnp.bfloat16),
            pltpu.VMEM((rows, LANES), jnp.bfloat16),
            pltpu.VMEM((rows, LANES), f32),
            pltpu.VMEM((2 * LANES, 3 * LANES), jnp.bfloat16),
            line,
            line,
            pltpu.VMEM((24, LANES), f32),
            pltpu.VMEM((8, cols), f32),
            pltpu.VMEM((24, LANES), f32),
            pltpu.VMEM((8, cols), f32),
            line,
            line,
            line,
            pltpu.VMEM((n_col, LANES), f32),
            pltpu.VMEM((n_row, LANES), f32),
            line,
            line,
            dma((len(PARTS),)),
            dma((4,)),
            dma((3,)),
            dma((3,)),
            pltpu.SemaphoreType.REGULAR((n_col,)),
            pltpu.SemaphoreType.REGULAR((n_row,)),
            dma((n_col,)),
            dma((n_col,)),
            dma((n_row,)),
            dma((n_row,)),
            dma((2,)),
        ],
        compiler_params=pltpu.CompilerParams(
            collective_id=0, has_side_effects=True, vmem_limit_bytes=24 * 1024 * 1024
        ),
    )(pltpu.with_memory_space_constraint(wrapped, pltpu.HBM), col_steps, row_steps)
    out = pl.pallas_call(
        add_offset,
        out_shape=jax.ShapeDtypeStruct((1, rows, cols), f32),
        in_specs=[in_vmem, in_vmem],
        out_specs=in_hbm,
        scratch_shapes=[pltpu.VMEM((rows, cols), f32), dma((PIECES,))],
        compiler_params=pltpu.CompilerParams(vmem_limit_bytes=8 * 1024 * 1024),
    )(pre, offset)
    return out


def solution(mesh):
    spec = P(None, "row", "col")
    return jax.shard_map(
        functools.partial(on_device, mesh.shape["row"], mesh.shape["col"]),
        mesh=mesh, in_specs=(spec, spec, spec), out_specs=spec, check_vma=False,
    )
```

```python
import functools
import math

import jax
import jax.numpy as jnp
from jax import lax
from jax.experimental import pallas as pl
from jax.experimental.pallas import tpu as pltpu
from jax.sharding import PartitionSpec as P

ITERS = 2
PER_CYCLE = 1.0 / (2.0 * math.pi)
MESH = pl.DeviceIdType.MESH
LANES = 128
STRIP = 16
PARTS = (256, 256, 256, 256)
MEET = 2
PIECES = 8
NEAR = 3
SIDE = 4


def turns(change):
    return jnp.floor(change * PER_CYCLE + 0.5)


def positions(shape):
    return lax.broadcasted_iota(jnp.int32, shape, 0), lax.broadcasted_iota(jnp.int32, shape, 1)


def before(line, first):
    sub, lane = positions(line.shape)
    along = pltpu.roll(line, 1, 1)
    moved = jnp.where(lane == 0, pltpu.roll(along, 1, 0), along)
    return jnp.where((lane == 0) & (sub == 0), first, moved)


def line_turns(line):
    return turns(line - before(line, line))


def edge_weight(inner, outer, inner_first, outer_first, no_first):
    sub, lane = positions(inner.shape)
    cross = turns(outer - inner)
    cross_before = before(cross, turns(outer_first - inner_first))
    along_inner = turns(inner - before(inner, inner_first))
    along_outer = turns(outer - before(outer, outer_first))
    charge = jnp.abs(cross_before - cross + along_outer - along_inner)
    charge = jnp.where((lane == 0) & (sub == 0) & no_first, 0.0, charge)
    return 1.0 / (1.0 + charge)


def total(x):
    return jnp.sum(jnp.sum(x, axis=1, keepdims=True), axis=0, keepdims=True)


def running_turns(lines):
    stack = jnp.concatenate([line_turns(v) for v in lines], axis=0)
    sub, _ = positions(stack.shape)
    sub = lax.rem(sub, 8)
    carry = jnp.where(sub >= 1, pltpu.roll(stack, 1, 0), 0.0)
    for step in (1, 2, 4):
        carry = carry + jnp.where(sub >= step, pltpu.roll(carry, step, 0), 0.0)
    ka, kb = positions((2 * LANES, LANES))
    prefix = jnp.dot(
        jnp.concatenate([stack, carry], axis=1).astype(jnp.bfloat16),
        ((ka <= kb) | (ka >= LANES)).astype(jnp.float32).astype(jnp.bfloat16),
        preferred_element_type=jnp.float32,
    )
    return [prefix[8 * k : 8 * k + 8] for k in range(len(lines))]


def row_line(ref, i):
    return jnp.concatenate([ref[i : i + 1, LANES * s : LANES * (s + 1)] for s in range(8)], axis=0)


def distance(t):
    return jnp.minimum(lax.div(t, SIDE), SIDE // 2) + jnp.minimum(lax.rem(t, SIDE), SIDE // 2)


def kernel(
    n_row, n_col, wrapped, col_steps, row_steps, pre, offset,
    x, sides, m, acc, mcol, tri, own_col, bottom, edge_x, edge_y, left, above, corner,
    jump_x, jump_y, seen_x, seen_y, first_x, first_y,
    in_sem, edge_sem, halo_send, halo_recv, ready_x, ready_y, x_send, x_recv, y_send, y_recv, first_recv,
):
    r, c = lax.axis_index("row"), lax.axis_index("col")
    rows, cols = x.shape
    blocks = cols // LANES
    src = wrapped.at[0]

    get_bottom = pltpu.make_async_copy(src.at[pl.ds(rows - 8, 8), :], edge_y, edge_sem.at[0])
    get_corner = pltpu.make_async_copy(
        src.at[pl.ds(rows - 8, 8), pl.ds(cols - LANES, LANES)], bottom, edge_sem.at[1]
    )
    get_parts = [
        pltpu.make_async_copy(
            src.at[pl.ds(sum(PARTS[:k]), part), :], x.at[pl.ds(sum(PARTS[:k]), part), :], in_sem.at[k]
        )
        for k, part in enumerate(PARTS)
    ]
    get_sides = [
        pltpu.make_async_copy(src.at[:, pl.ds(at, LANES)], sides.at[k], edge_sem.at[2 + k])
        for k, at in enumerate((0, cols - LANES))
    ]
    for copy in [get_sides[0]] + get_parts[:MEET] + [get_bottom, get_corner] + get_parts[MEET:] + [get_sides[1]]:
        copy.start()

    barrier = pltpu.get_barrier_semaphore()

    def greet(device):
        pl.semaphore_signal(barrier, inc=1, device_id=device, device_id_type=MESH)

    away = distance(r)
    row_distance = [min(t // SIDE, SIDE // 2) + min(t % SIDE, SIDE // 2) for t in range(n_row)]
    from_low = [(t < r) & (row_distance[t] <= away) for t in range(n_row)]

    @pl.when(c > 0)
    def _():
        greet({"col": c - 1})

    @pl.when((r > 0) & (c > 0))
    def _():
        greet({"row": r - 1, "col": c - 1})

    for t in range(n_row):
        greets_low = (t < r) & ((t == r - 1) | (row_distance[t] > away))

        @pl.when(greets_low | ((t > r) & (row_distance[t] >= away)))
        def _(t=t):
            greet({"row": t})

    @pl.loop(c + 1, n_col)
    def _(t):
        greet({"col": t})

    has_right, has_below = c < n_col - 1, r < n_row - 1
    expected = c + has_right.astype(jnp.int32) + (has_right & has_below).astype(jnp.int32)
    for t in range(n_row):
        from_high = (t == r + 1) | ((t > r) & (row_distance[t] < away))
        expected = expected + (from_low[t] | from_high).astype(jnp.int32)

    def meet():
        get_bottom.wait()
        get_corner.wait()
        down_total = down[7:8, LANES - 1 : LANES] - row_steps[0, 0, 0].astype(jnp.float32)
        for s in range(8):
            edge_y[5:6, LANES * s : LANES * (s + 1)] = jnp.broadcast_to(down_total, (1, LANES))
        pl.semaphore_wait(barrier, expected)

        @pl.when(has_below)
        def _():
            to_below.start()

        @pl.when(has_right & has_below)
        def _():
            to_both.start()

        for t in reversed(range(n_row)):
            @pl.when(from_low[t] & (t != r - 1))
            def _(t=t):
                pl.semaphore_signal(ready_y.at[r], inc=1, device_id={"row": t}, device_id_type=MESH)

        @pl.loop(1, c)
        def _(k):
            pl.semaphore_signal(
                ready_x.at[c], inc=1, device_id={"col": c - 1 - k}, device_id_type=MESH
            )

    get_sides[0].wait()
    for s in range(8):
        own_col[pl.ds(s, 1), :] = sides[0, pl.ds(LANES * s, LANES), :].T[0:1, :]
    (down,) = running_turns([own_col[...]])
    def halo(src_ref, dst_ref, k, device):
        return pltpu.make_async_remote_copy(
            src_ref=src_ref, dst_ref=dst_ref, send_sem=halo_send.at[k], recv_sem=halo_recv.at[k],
            device_id=device, device_id_type=MESH,
        )

    next_row, next_col = lax.rem(r + 1, n_row), lax.rem(c + 1, n_col)
    to_right = halo(edge_x, left, 0, {"col": next_col})
    to_below = halo(edge_y.at[pl.ds(5, 3), :], above.at[pl.ds(5, 3), :], 1, {"row": next_row})
    to_both = halo(bottom, corner, 2, {"row": next_row, "col": next_col})
    sends = ((has_below, to_below), (has_right, to_right), (has_right & has_below, to_both))
    arrivals = ((r > 0, to_below), (c > 0, to_right), ((r > 0) & (c > 0), to_both))

    first = 0
    for k, part in enumerate(PARTS):
        if k == MEET:
            meet()
        get_parts[k].wait()
        for q in range(first // STRIP, (first + part) // STRIP):
            at = pl.ds(STRIP * q, STRIP)
            lane = lax.broadcasted_iota(jnp.int32, (STRIP, LANES), 1)
            counts, moved = [], None
            for j in range(blocks):
                here = x[at, pl.ds(LANES * j, LANES)]
                last, moved = moved, pltpu.roll(here, 1, 1)
                back = moved if j == 0 else jnp.where(lane == 0, last, moved)
                n = turns(here - back)
                n = jnp.where(lane == 0, 0.0, n) if j == 0 else n
                m[j, at, :] = n.astype(jnp.bfloat16)
                counts.append(n)
            while len(counts) > 1:
                counts = [a + b for a, b in zip(counts[::2], counts[1::2])]
            acc[at, :] = counts[0].astype(jnp.bfloat16)
        first += part

    get_sides[1].wait()
    for s in range(8):
        turned = sides[1, pl.ds(LANES * s, LANES), :].T
        edge_x[pl.ds(s, 1), :] = turned[LANES - 2 : LANES - 1, :]
        edge_x[pl.ds(8 + s, 1), :] = turned[LANES - 1 : LANES, :]

    sub, lane = positions((8, LANES))
    flat_totals = lax.dot_general(
        jnp.ones((8, LANES), jnp.bfloat16), acc[...], (((1,), (1,)), ((), ())),
        preferred_element_type=jnp.float32,
    )
    row_totals = jnp.zeros((8, LANES), jnp.float32)
    for s in range(8):
        row_totals = jnp.where(sub == s, flat_totals[:, LANES * s : LANES * (s + 1)], row_totals)
    edge_x[16:24, :] = down + row_totals - col_steps[0, 0, 0].astype(jnp.float32)
    @pl.when(has_right)
    def _():
        to_right.start()

    for holds, copy in arrivals:
        @pl.when(holds)
        def _(copy=copy):
            copy.wait_recv()

    col0, row0 = own_col[...], row_line(x, 0)
    col_in, col_out = left[0:8, :], left[8:16, :]
    row_in, row_out = row_line(above, 6), row_line(above, 7)
    weight_x = edge_weight(
        col_in, col_out, corner[7:8, LANES - 2 : LANES - 1], corner[7:8, LANES - 1 : LANES], r == 0
    )
    weight_y = edge_weight(
        row_in, row_out, corner[6:7, LANES - 1 : LANES], corner[7:8, LANES - 1 : LANES], c == 0
    )
    along, along_above = running_turns([row0, row_out])
    miss_x = down - left[16:24, :] - turns(col0 - col_out)
    miss_y = along - along_above - above[5:6, 0:LANES] - turns(row0 - row_out)
    mean_x = total(weight_x * miss_x) / total(weight_x)
    mean_y = total(weight_y * miss_y) / total(weight_y)
    jump_x[...] = jnp.broadcast_to(jnp.where(c == 0, 0.0, mean_x), (8, LANES))
    jump_y[...] = jnp.broadcast_to(jnp.where(r == 0, 0.0, mean_y), (8, LANES))

    def to_row(t):
        return pltpu.make_async_remote_copy(
            src_ref=jump_y.at[pl.ds(0, 1), :], dst_ref=seen_y.at[pl.ds(r, 1), :],
            send_sem=y_send.at[t], recv_sem=y_recv.at[r],
            device_id={"row": t}, device_id_type=MESH,
        )

    def to_col(t):
        return pltpu.make_async_remote_copy(
            src_ref=jump_x.at[pl.ds(0, 1), :], dst_ref=seen_x.at[pl.ds(c, 1), :],
            send_sem=x_send.at[t], recv_sem=x_recv.at[c],
            device_id={"col": t}, device_id_type=MESH,
        )

    def from_row(k):
        return pltpu.make_async_remote_copy(
            src_ref=jump_y.at[pl.ds(0, 1), :], dst_ref=seen_y.at[pl.ds(k, 1), :],
            send_sem=y_send.at[k], recv_sem=y_recv.at[k],
            device_id={"row": k}, device_id_type=MESH,
        )

    def from_col(k):
        return pltpu.make_async_remote_copy(
            src_ref=jump_x.at[pl.ds(0, 1), :], dst_ref=seen_x.at[pl.ds(k, 1), :],
            send_sem=x_send.at[k], recv_sem=x_recv.at[k],
            device_id={"col": k}, device_id_type=MESH,
        )

    def first_row(t):
        return pltpu.make_async_remote_copy(
            src_ref=jump_y.at[pl.ds(0, 1), :], dst_ref=first_y.at[pl.ds(0, 1), :],
            send_sem=y_send.at[t], recv_sem=first_recv.at[0],
            device_id={"row": t}, device_id_type=MESH,
        )

    def first_col(t):
        return pltpu.make_async_remote_copy(
            src_ref=jump_x.at[pl.ds(0, 1), :], dst_ref=first_x.at[pl.ds(0, 1), :],
            send_sem=x_send.at[t], recv_sem=first_recv.at[1],
            device_id={"col": t}, device_id_type=MESH,
        )

    def await_y(t):
        @pl.when((t > r + 1) & (away <= distance(t)))
        def _():
            pl.semaphore_wait(ready_y.at[t], 1)

    def await_x(t):
        @pl.when(t > c + 1)
        def _():
            pl.semaphore_wait(ready_x.at[t], 1)

    def send_y(t):
        await_y(t)
        to_row(t).start()

    def send_x(t):
        await_x(t)
        to_col(t).start()

    stop_x = jnp.where(c < n_col // 4, n_col // 2, n_col)
    start_y, start_x = jnp.where(r == 0, n_row, r + 1), jnp.where(c == 0, stop_x, c + 1)
    near_y, near_x = jnp.minimum(start_y + NEAR, n_row), jnp.minimum(start_x + NEAR, stop_x)
    pl.loop(start_y, near_y)(send_y)
    pl.loop(start_x, near_x)(send_x)
    late_x = jnp.where(c < n_col // 2, near_x, stop_x)
    pl.loop(near_x, late_x)(send_x)
    pl.loop(near_y, n_row)(send_y)

    for s in range(8):
        mcol[pl.ds(LANES * s, LANES), :] = jnp.broadcast_to(down[s : s + 1, :], (LANES, LANES)).T
    ta, tb = positions(tri.shape)
    tri[...] = ((ta <= tb) | (tb >= 2 * LANES)).astype(jnp.float32).astype(jnp.bfloat16)

    @pl.loop(0, rows // 256)
    def _(k):
        at = pl.ds(pl.multiple_of(k * 256, 256), 256)
        base = mcol[at, :]
        for j in range(blocks // 2):
            counted = jnp.dot(
                jnp.concatenate([m[2 * j, at, :], m[2 * j + 1, at, :]], axis=1), tri[...],
                preferred_element_type=jnp.float32,
            )
            for h in range(2):
                here = pl.ds(LANES * (2 * j + h), LANES)
                pre[at, here] = x[at, here] * PER_CYCLE - counted[:, LANES * h : LANES * (h + 1)] - base
            base = base + counted[:, 2 * LANES :]

    pl.loop(late_x, stop_x)(send_x)

    @pl.loop(1, r)
    def _(k):
        from_row(k).wait_recv()

    @pl.loop(1, c)
    def _(k):
        from_col(k).wait_recv()

    seen = lax.broadcasted_iota(jnp.int32, (n_col, LANES), 0)
    across = jnp.sum(jnp.where((seen > 0) & (seen < c), seen_x[...], 0.0), axis=0, keepdims=True) + jump_x[0:1, :]
    seen = lax.broadcasted_iota(jnp.int32, (n_row, LANES), 0)
    downs = jnp.sum(jnp.where((seen > 0) & (seen < r), seen_y[...], 0.0), axis=0, keepdims=True) + jump_y[0:1, :]

    @pl.when(r == 0)
    def _():
        jump_y[...] = jnp.broadcast_to(across, (8, LANES))

        @pl.loop(1, n_row)
        def _(t):
            await_y(t)
            first_row(t).start()

    @pl.when(c == 0)
    def _():
        jump_x[...] = jnp.broadcast_to(downs, (8, LANES))

        @pl.loop(1, n_col)
        def _(t):
            await_x(t)
            first_col(t).start()

    @pl.when(c > 0)
    def _():
        pl.loop(stop_x, n_col)(send_x)

    @pl.when(r > 0)
    def _():
        first_row(0).wait_recv()

    @pl.when(c > 0)
    def _():
        first_col(0).wait_recv()

    across_top = jnp.where(r == 0, across, first_y[0:1, :])
    downs_left = jnp.where(c == 0, downs, first_x[0:1, :])

    mine = top_tile = left_tile = origin = jnp.zeros((1, LANES), jnp.float32)
    for sweep in range(ITERS):
        prefix_across = across + left_tile - mine
        prefix_across_top = across_top + origin - top_tile
        prefix_down = downs + top_tile - mine
        prefix_down_left = downs_left + origin - left_tile
        mine = mine + 0.5 * (prefix_across + prefix_across_top + prefix_down + prefix_down_left)
        top_tile = top_tile + 0.5 * (prefix_across_top + prefix_across_top)
        left_tile = left_tile + 0.5 * (prefix_down_left + prefix_down_left)
    offset[...] = jnp.broadcast_to(mine, (8, LANES))

    for holds, copy in sends:
        @pl.when(holds)
        def _(copy=copy):
            copy.wait_send()

    @pl.loop(r + 1, n_row)
    def _(t):
        to_row(t).wait_send()

    @pl.loop(c + 1, n_col)
    def _(t):
        to_col(t).wait_send()


def add_offset(pre, offset, out, done, sem):
    piece = pre.shape[0] // PIECES
    copies = []
    for k in range(PIECES):
        at = pl.ds(k * piece, piece)
        done[at, :] = pre[at, :] + offset[0:1, 0:1]
        copy = pltpu.make_async_copy(done.at[at, :], out.at[0, at, :], sem.at[k])
        copy.start()
        copies.append(copy)
    for copy in copies:
        copy.wait()


def on_device(n_row, n_col, wrapped, col_steps, row_steps):
    _, rows, cols = wrapped.shape
    f32 = jnp.float32
    line = pltpu.VMEM((8, LANES), f32)
    dma = pltpu.SemaphoreType.DMA
    in_hbm = pl.BlockSpec(memory_space=pltpu.HBM)
    in_smem = pl.BlockSpec(memory_space=pltpu.SMEM)
    in_vmem = pl.BlockSpec(memory_space=pltpu.VMEM)
    pre, offset = pl.pallas_call(
        functools.partial(kernel, n_row, n_col),
        out_shape=(jax.ShapeDtypeStruct((rows, cols), f32), jax.ShapeDtypeStruct((8, LANES), f32)),
        in_specs=[in_hbm, in_smem, in_smem],
        out_specs=(in_vmem, in_vmem),
        scratch_shapes=[
            pltpu.VMEM((rows, cols), f32),
            pltpu.VMEM((2, rows, LANES), f32),
            pltpu.VMEM((cols // LANES, rows, LANES), jnp.bfloat16),
            pltpu.VMEM((rows, LANES), jnp.bfloat16),
            pltpu.VMEM((rows, LANES), f32),
            pltpu.VMEM((2 * LANES, 3 * LANES), jnp.bfloat16),
            line,
            line,
            pltpu.VMEM((24, LANES), f32),
            pltpu.VMEM((8, cols), f32),
            pltpu.VMEM((24, LANES), f32),
            pltpu.VMEM((8, cols), f32),
            line,
            line,
            line,
            pltpu.VMEM((n_col, LANES), f32),
            pltpu.VMEM((n_row, LANES), f32),
            line,
            line,
            dma((len(PARTS),)),
            dma((4,)),
            dma((3,)),
            dma((3,)),
            pltpu.SemaphoreType.REGULAR((n_col,)),
            pltpu.SemaphoreType.REGULAR((n_row,)),
            dma((n_col,)),
            dma((n_col,)),
            dma((n_row,)),
            dma((n_row,)),
            dma((2,)),
        ],
        compiler_params=pltpu.CompilerParams(
            collective_id=0, has_side_effects=True, vmem_limit_bytes=24 * 1024 * 1024
        ),
    )(pltpu.with_memory_space_constraint(wrapped, pltpu.HBM), col_steps, row_steps)
    out = pl.pallas_call(
        add_offset,
        out_shape=jax.ShapeDtypeStruct((1, rows, cols), f32),
        in_specs=[in_vmem, in_vmem],
        out_specs=in_hbm,
        scratch_shapes=[pltpu.VMEM((rows, cols), f32), dma((PIECES,))],
        compiler_params=pltpu.CompilerParams(vmem_limit_bytes=8 * 1024 * 1024),
    )(pre, offset)
    return out


def solution(mesh):
    spec = P(None, "row", "col")
    return jax.shard_map(
        functools.partial(on_device, mesh.shape["row"], mesh.shape["col"]),
        mesh=mesh, in_specs=(spec, spec, spec), out_specs=spec, check_vma=False,
    )
```
